32 devices in a mesh: parts: 2 (over x), row: 8 (over z, y), col: 2 (over core).
Axes of the slice: x: 2, y: 2, z: 4, core: 2. Of those that a mesh axis runs over, the one named last changes fastest.
Arguments:
- tokens: bfloat16 [64, 512, 512], P(('parts', 'row'), 'col'), parts along dimension 0, may hold values from -6 to 6
- expand_weight: bfloat16 [512, 2048], replicated, may hold values from -0.25 to 0.25
- depth_kernel: float32 [3, 3, 2048], replicated, may hold values from -2 to 2
- project_weight: bfloat16 [2048, 512], replicated, may hold values from -0.125 to 0.125
- norm_gain: float32 [512], replicated, may hold values from 0.25 to 1.75
- attend_weight: bfloat16 [512, 1536], replicated, may hold values from -3 to 3
- output_weight: bfloat16 [512, 512], replicated, may hold values from -0.25 to 0.25
Outputs:
- section_out: bfloat16 [64, 512, 512], P(('parts', 'row'), 'col'), parts along dimension 0
The draws below stay inside these ranges and needn't reach their ends.
There are 2 independent parts, one for each index of `parts`. The reference program is written for one: setup_inputs(seed, part) draws one part's arguments, and reference() takes and returns one part's arrays. A program takes and returns all parts, laid end to end along the dimension named above; an argument that names none is the same for every part. Nothing has to cross between parts.
All inputs are finite; a program needn't handle non-finite values.
Results may differ from the reference program's by a relative error of at most 0.012.
Values may be sent and summed in bfloat16 or wider, within the bound.
No kernel may reach another device: no remote copies, remote signals or barrier semaphores. Data moves between devices by JAX's collectives and lax.ppermute only.
A program may use at most 128 MiB of HBM per device.

```python
import math
import jax
import jax.numpy as jnp
from jax import lax

C = 512
HID = 2048
HEADS = 16
HEAD_DIM = 32
GRID = 16
TILE_ROWS = 4
H = 32
W = 512


def draw_attend_weight(key, part):
    first, second, third = jax.random.split(key, 3)
    queries = jax.random.normal(first, (C, C), jnp.float32) * 1.5 / math.sqrt(C)
    keyed = jax.random.normal(second, (C, C), jnp.float32) * 1.5 / math.sqrt(C)
    values = jax.random.normal(third, (C, C), jnp.float32) * 2.0 / math.sqrt(C)
    whole = jnp.concatenate([queries, keyed, values], axis=1)
    return jnp.clip(whole, -3.0, 3.0).astype(jnp.bfloat16)


def shard_levels(rng, dims, cuts, low, largest):
    level, own = 1.0, jax.random.fold_in(rng, 6)
    for axis_at, parts in cuts:
        steps = jnp.exp(jax.random.uniform(jax.random.fold_in(own, axis_at), (parts,), jnp.float32, low / len(cuts), largest / len(cuts)))
        level = level * jnp.repeat(steps, dims[axis_at] // parts).reshape([-1 if axis == axis_at else 1 for axis in range(len(dims))])
    return level


def noise(own_key, dims, scale, limit, cuts=(), kind=jnp.bfloat16):
    level = shard_levels(own_key, dims, cuts, -0.22, 0.18) if cuts else 1.0
    values = jax.random.normal(own_key, dims, jnp.float32) * scale * level
    return jnp.minimum(jnp.maximum(values, -limit), limit).astype(kind)


def setup_inputs(seed: int = 0, part: int = 0) -> dict:
    keys = jax.random.split(jax.random.key(seed), 8)
    part_keys = jax.random.split(jax.random.fold_in(keys[7], part), 8)
    return {
        "tokens": noise(part_keys[0], (H, W, C), 1.0, 6.0, ((0, 8), (1, 2))),
        "expand_weight": noise(keys[1], (C, HID), C ** -0.5, 0.25),
        "depth_kernel": noise(keys[2], (3, 3, HID), 9 ** -0.5, 2.0, (), jnp.float32),
        "project_weight": noise(keys[3], (HID, C), HID ** -0.5, 0.125),
        "norm_gain": jnp.clip(1.0 + 0.15 * jax.random.normal(keys[4], (C,), jnp.float32), 0.25, 1.75),
        "attend_weight": draw_attend_weight(jax.random.fold_in(keys[7], 71), part),
        "output_weight": noise(keys[6], (C, C), C ** -0.5, 0.25),
    }


def gelu_tanh(values):
    return jax.nn.gelu(values, approximate=True)

def mbconv_region(tokens, expand_weight, depth_kernel, project_weight):
    height, width, channels = tokens.shape
    padded = jnp.pad(tokens, ((1, 1), (1, 1), (0, 0)))
    block = TILE_ROWS

    def one_block(index):
        start = (index * block).astype(jnp.int32)
        window = lax.dynamic_slice_in_dim(padded, start, block + 2, 0)
        product = jnp.dot(window.reshape(-1, channels), expand_weight, preferred_element_type=jnp.float32)
        expanded = gelu_tanh(product).astype(jnp.bfloat16).reshape(block + 2, width + 2, -1)
        total = jnp.zeros((block, width, expanded.shape[2]), jnp.float32)
        for shift_row in range(3):
            for shift_col in range(3):
                total = total + expanded[shift_row:shift_row + block, shift_col:shift_col + width].astype(jnp.float32) * depth_kernel[shift_row, shift_col]
        depth = gelu_tanh(total).astype(jnp.bfloat16)
        center = lax.dynamic_slice_in_dim(tokens, start, block, 0)
        branch = jnp.dot(depth.reshape(block * width, -1), project_weight, preferred_element_type=jnp.float32)
        return (center.astype(jnp.float32) + branch.reshape(block, width, channels)).astype(jnp.bfloat16)
    blocks = lax.map(one_block, jnp.arange(height // block, dtype=jnp.int32))
    return blocks.reshape(height, width, channels)

def layer_norm(values, gain):
    values = values.astype(jnp.float32)
    center = lax.optimization_barrier(jnp.mean(values, axis=-1, keepdims=True))
    spread = lax.optimization_barrier(jnp.mean((values - center) ** 2, axis=-1, keepdims=True))
    return ((values - center) * lax.rsqrt(spread + 1e-05) * gain).astype(jnp.bfloat16)

def attend_groups(groups, attend_weight, output_weight):
    count, members, channels = groups.shape
    projected = jnp.dot(groups.reshape(count * members, channels), attend_weight, preferred_element_type=jnp.float32)
    projected = projected.astype(jnp.bfloat16).reshape(count, members, 3, HEADS, HEAD_DIM)
    query_heads = projected[:, :, 0].astype(jnp.float32)
    key_heads = projected[:, :, 1].astype(jnp.float32)
    value_heads = projected[:, :, 2].astype(jnp.float32)
    scores = jnp.einsum('nqhd,nkhd->nhqk', query_heads, key_heads) / math.sqrt(HEAD_DIM)
    soft = jax.nn.softmax(scores, axis=-1).astype(jnp.bfloat16)
    heads_out = jnp.einsum('nhqk,nkhd->nqhd', soft.astype(jnp.float32), value_heads)
    heads_out = heads_out.astype(jnp.bfloat16).reshape(count * members, channels)
    result = jnp.dot(heads_out, output_weight, preferred_element_type=jnp.float32).astype(jnp.bfloat16)
    return result.reshape(count, members, channels)

def reference(tokens, expand_weight, depth_kernel, project_weight, norm_gain, attend_weight, output_weight):
    height, width, channels = tokens.shape
    mbconv = mbconv_region(tokens, expand_weight, depth_kernel, project_weight)
    normed = layer_norm(mbconv, norm_gain)
    stride_rows = height // GRID
    stride_cols = width // GRID
    grouped = normed.reshape(GRID, stride_rows, GRID, stride_cols, channels).transpose(1, 3, 0, 2, 4)
    group_total = stride_rows * stride_cols
    block = math.gcd(group_total, 8)
    grouped = grouped.reshape(group_total // block, block, GRID * GRID, channels)
    attended = lax.map(lambda part_groups: attend_groups(part_groups, attend_weight, output_weight), grouped)
    attended = attended.reshape(stride_rows, stride_cols, GRID, GRID, channels).transpose(2, 0, 3, 1, 4)
    attention = attended.reshape(height, width, channels)
    return (mbconv.astype(jnp.float32) + attention.astype(jnp.float32)).astype(jnp.bfloat16)
```

```python
import functools
import math

import jax
import jax.numpy as jnp
from jax import lax
from jax.experimental import pallas as pl
from jax.experimental.pallas import tpu as pltpu
from jax.sharding import PartitionSpec as P

HEADS = 16
HEAD_DIM = 32
GRID = 16
CHUNKS = 2
SUBLANES = 8
LANES = 128
LOG2E = 1.4426950408889634


def extended(cells, sides, width):
    for axis, dim in sides:
        count = lax.axis_size(axis)
        ends = count - 1
        head = lax.slice_in_dim(cells, 0, width, axis=dim)
        tail = lax.slice_in_dim(cells, cells.shape[dim] - width, cells.shape[dim], axis=dim)
        cells = jnp.concatenate(
            [
                lax.ppermute(tail, axis, [(i, (i + 1) % count) for i in range(ends)]),
                cells,
                lax.ppermute(head, axis, [((i + 1) % count, i) for i in range(ends)]),
            ],
            axis=dim,
        )
    return cells


def gelu_tanh(values):
    return jax.nn.gelu(values, approximate=True)


def gelu_fast(v):
    inner = v * (0.7978845608028654 + (0.7978845608028654 * 0.044715) * (v * v))
    half = 0.5 * v
    return half + half * jnp.tanh(inner)


def expand_tile(inputs, expand_weight):
    shape = inputs.shape
    product = jnp.dot(
        inputs.reshape(-1, shape[2]), expand_weight, preferred_element_type=jnp.float32
    )
    return gelu_tanh(product).astype(jnp.bfloat16).reshape(shape[0], shape[1], -1)


def layer_norm(values, gain):
    values = values.astype(jnp.float32)
    center = jnp.mean(values, axis=-1, keepdims=True)
    spread = jnp.mean((values - center) ** 2, axis=-1, keepdims=True)
    return ((values - center) * lax.rsqrt(spread + 1e-05) * gain).astype(jnp.bfloat16)


def attend_groups(groups, attend_weight, output_weight):
    count, members, channels = groups.shape
    projected = jnp.dot(
        groups.reshape(count * members, channels), attend_weight, preferred_element_type=jnp.float32
    )
    projected = projected.astype(jnp.bfloat16).reshape(count, members, 3, HEADS, HEAD_DIM)
    query_heads = projected[:, :, 0]
    key_heads = projected[:, :, 1]
    value_heads = projected[:, :, 2]
    scores = jnp.einsum(
        "nqhd,nkhd->nhqk", query_heads, key_heads, preferred_element_type=jnp.float32
    ) / math.sqrt(HEAD_DIM)
    soft = jax.nn.softmax(scores, axis=-1).astype(jnp.bfloat16)
    heads_out = jnp.einsum("nhqk,nkhd->nqhd", soft, value_heads, preferred_element_type=jnp.float32)
    heads_out = heads_out.astype(jnp.bfloat16).reshape(count * members, channels)
    result = jnp.dot(heads_out, output_weight, preferred_element_type=jnp.float32).astype(
        jnp.bfloat16
    )
    return result.reshape(count, members, channels)


def mbconv_kernel(
    col_ref, x_ref, up_ref, down_ref, side_ref, side_up_ref, side_down_ref,
    expand_ref, taps_ref, project_ref, gain_ref,
    normed_ref, mbconv_ref,
    ordered, expanded, depth, acc,
    *, chunk, span, stride_cols, stride_rows,
):
    step = pl.program_id(0)
    rows, cols, channels = x_ref.shape
    blocks = cols // stride_cols
    wide = span + 2
    size = wide * blocks
    hidden = expand_ref.shape[1]
    row_blocks = rows // stride_rows
    first = chunk * span == 0
    last = (chunk + 1) * span == stride_cols

    @pl.when(step == 0)
    def _():
        at = lax.broadcasted_iota(jnp.int32, (size, cols), 0)
        want = (at % blocks) * stride_cols + at // blocks + (chunk * span - 1)
        select = (lax.broadcasted_iota(jnp.int32, (size, cols), 1) == want).astype(jnp.bfloat16)
        position = lax.broadcasted_iota(jnp.int32, (size, channels), 0)
        is_left = col_ref[0] == 0
        for row in range(rows + 2):
            if row == 0:
                source, edge = up_ref[0], side_up_ref[...]
            elif row == rows + 1:
                source, edge = down_ref[0], side_down_ref[...]
            else:
                source, edge = x_ref[row - 1], side_ref[row - 1 : row, :]
            picked = jnp.dot(select, source, preferred_element_type=jnp.float32)
            edge = edge.astype(jnp.float32)
            zero = jnp.zeros_like(edge)
            if first:
                picked = jnp.where(position == 0, jnp.where(is_left, zero, edge), picked)
            if last:
                picked = jnp.where(position == size - 1, jnp.where(is_left, edge, zero), picked)
            ordered[row] = picked.astype(jnp.bfloat16)

    for row in range(rows + 2):
        product = jnp.dot(ordered[row], expand_ref[...], preferred_element_type=jnp.float32)
        expanded[row] = gelu_fast(product).reshape(wide, blocks, hidden)

    for lane in range(0, hidden, LANES):
        taps = [
            [taps_ref[3 * dr + dc : 3 * dr + dc + 1, lane : lane + LANES] for dc in range(3)]
            for dr in range(3)
        ]
        for b in range(span):
            for hm in range(stride_rows):
                parts = []
                for rb in range(row_blocks):
                    row = rb * stride_rows + hm
                    total = None
                    for dr in range(3):
                        for dc in range(3):
                            term = expanded[row + dr, b + dc, :, lane : lane + LANES] * taps[dr][dc]
                            total = term if total is None else total + term
                    parts.append(gelu_fast(total))
                place = (hm * span + b) * row_blocks * blocks
                depth[place : place + row_blocks * blocks, lane : lane + LANES] = jnp.concatenate(
                    parts, axis=0
                ).astype(jnp.bfloat16)

    branch = jnp.dot(depth[...], project_ref[...], preferred_element_type=jnp.float32)

    @pl.when(step == 0)
    def _():
        acc[...] = branch

    @pl.when(step > 0)
    def _():
        acc[...] = acc[...] + branch

    @pl.when(step == pl.num_programs(0) - 1)
    def _():
        gain = gain_ref[...]
        members = row_blocks * blocks
        for hm in range(stride_rows):
            for b in range(span):
                pieces = []
                for rb in range(row_blocks):
                    begin = (b + 1) * blocks
                    low = begin - begin % 16
                    pair = ordered[rb * stride_rows + hm + 1, low : low + 16, :].astype(jnp.float32)
                    pieces.append(pair[begin - low : begin - low + blocks])
                place = (hm * span + b) * members
                mixed = jnp.concatenate(pieces, axis=0) + acc[place : place + members, :]
                mixed = mixed.astype(jnp.bfloat16)
                mbconv_ref[place : place + members, :] = mixed
                mixed = mixed.astype(jnp.float32)
                center = jnp.mean(mixed, axis=-1, keepdims=True)
                moved = mixed - center
                spread = jnp.mean(moved * moved, axis=-1, keepdims=True)
                normed_ref[place : place + members, :] = (
                    moved * lax.rsqrt(spread + 1e-05) * gain
                ).astype(jnp.bfloat16)


def mbconv_chunk(chunk, span, stride_rows, stride_cols, col, tokens, halos, weights):
    rows, cols, channels = tokens.shape
    expand_weight, taps, project_weight, gain = weights
    hidden = expand_weight.shape[1]
    block = 256 if hidden % 256 == 0 else hidden
    blocks = cols // stride_cols
    count = rows * span * blocks
    size = (span + 2) * blocks

    def whole(array):
        return pl.BlockSpec(array.shape, lambda i, c: (0,) * array.ndim)

    grid_spec = pltpu.PrefetchScalarGridSpec(
        num_scalar_prefetch=1,
        grid=(hidden // block,),
        in_specs=[whole(tokens)]
        + [whole(h) for h in halos]
        + [
            pl.BlockSpec((channels, block), lambda i, c: (0, i)),
            pl.BlockSpec((taps.shape[0], block), lambda i, c: (0, i)),
            pl.BlockSpec((block, channels), lambda i, c: (i, 0)),
            whole(gain),
        ],
        out_specs=[pl.BlockSpec((count, channels), lambda i, c: (0, 0))] * 2,
        scratch_shapes=[
            pltpu.VMEM((rows + 2, size, channels), jnp.bfloat16),
            pltpu.VMEM((rows + 2, span + 2, blocks, block), jnp.float32),
            pltpu.VMEM((count, block), jnp.bfloat16),
            pltpu.VMEM((count, channels), jnp.float32),
        ],
    )
    return pl.pallas_call(
        functools.partial(
            mbconv_kernel, chunk=chunk, span=span, stride_cols=stride_cols, stride_rows=stride_rows
        ),
        grid_spec=grid_spec,
        out_shape=[jax.ShapeDtypeStruct((count, channels), jnp.bfloat16)] * 2,
        compiler_params=pltpu.CompilerParams(dimension_semantics=("arbitrary",)),
        cost_estimate=pl.CostEstimate(
            flops=4 * count * channels * hidden * 2, bytes_accessed=8 << 20, transcendentals=0
        ),
        name=f"mbconv_{chunk}",
    )(col, tokens, *halos, expand_weight, taps, project_weight, gain)


def attend_kernel(x_ref, attend_ref, output_ref, out_ref):
    sources, per, channels = x_ref.shape
    members = sources * per
    x = x_ref[...].reshape(members, channels)
    scale = LOG2E / math.sqrt(HEAD_DIM)
    fold = LANES // HEAD_DIM
    lane = lax.broadcasted_iota(jnp.int32, (members, LANES), 1) // HEAD_DIM
    ones = jnp.ones((members, LANES), jnp.bfloat16)
    tiles = []
    for tile in range(channels // LANES):
        begin = tile * LANES
        query = jnp.dot(
            x, attend_ref[:, begin : begin + LANES], preferred_element_type=jnp.float32
        )
        query = (query * scale).astype(jnp.bfloat16)
        key = jnp.dot(
            x,
            attend_ref[:, channels + begin : channels + begin + LANES],
            preferred_element_type=jnp.float32,
        ).astype(jnp.bfloat16)
        value = jnp.dot(
            x,
            attend_ref[:, 2 * channels + begin : 2 * channels + begin + LANES],
            preferred_element_type=jnp.float32,
        ).astype(jnp.bfloat16)
        upper = None
        for head in range(fold):
            inside = lane == head
            key_head = jnp.where(inside, key, jnp.zeros_like(key))
            value_head = jnp.where(inside, value, jnp.zeros_like(value))
            scores = lax.dot_general(
                query, key_head, (((1,), (1,)), ((), ())), preferred_element_type=jnp.float32
            )
            top = jnp.max(scores, axis=-1, keepdims=True)
            weight = jnp.exp2(scores - top).astype(jnp.bfloat16)
            mixed = jnp.dot(
                weight,
                jnp.concatenate([value_head, ones], axis=1),
                preferred_element_type=jnp.float32,
            )
            if upper is None:
                upper, lower = mixed[:, :LANES], mixed[:, LANES:]
            else:
                upper = upper + mixed[:, :LANES]
                lower = jnp.where(inside, mixed[:, LANES:], lower)
        tiles.append((upper / lower).astype(jnp.bfloat16))
    heads_out = jnp.concatenate(tiles, axis=1)
    result = jnp.dot(heads_out, output_ref[...], preferred_element_type=jnp.float32)
    out_ref[...] = result.astype(jnp.bfloat16).reshape(sources, per, channels)


def attend_chunk(chunk, piece, per, attend_weight, output_weight):
    sources, length, channels = piece.shape
    items = length // per
    members = sources * per
    spec = pl.BlockSpec((sources, per, channels), lambda i: (0, i, 0))
    return pl.pallas_call(
        attend_kernel,
        grid=(items,),
        in_specs=[
            spec,
            pl.BlockSpec(attend_weight.shape, lambda i: (0, 0)),
            pl.BlockSpec(output_weight.shape, lambda i: (0, 0)),
        ],
        out_specs=spec,
        out_shape=jax.ShapeDtypeStruct(piece.shape, jnp.bfloat16),
        compiler_params=pltpu.CompilerParams(dimension_semantics=("arbitrary",)),
        cost_estimate=pl.CostEstimate(
            flops=items * members * channels * (8 * channels + 8 * members),
            bytes_accessed=4 << 20,
            transcendentals=0,
        ),
        name=f"attend_{chunk}",
    )(piece, attend_weight, output_weight)


def finish_kernel(*refs, span, stride_rows, row_blocks, blocks):
    back_ref, mbconv_ref, out_ref = refs[0], refs[1], refs[-1]
    channels = back_ref.shape[-1]
    length = span * row_blocks * blocks
    total = back_ref[...].reshape(-1, channels).astype(jnp.float32) + mbconv_ref[...].astype(
        jnp.float32
    )
    total = total.astype(jnp.bfloat16)
    at = lax.broadcasted_iota(jnp.int32, (length, length), 0)
    b = at % span
    a = (at // span) % blocks
    rb = at // (span * blocks)
    select = lax.broadcasted_iota(jnp.int32, (length, length), 1) == (b * row_blocks + rb) * blocks + a
    select = select.astype(jnp.bfloat16)
    for hm in range(stride_rows):
        placed = jnp.dot(
            select, total[hm * length : (hm + 1) * length], preferred_element_type=jnp.float32
        ).astype(jnp.bfloat16)
        for rb_at in range(row_blocks):
            out_ref[rb_at * stride_rows + hm] = placed[
                rb_at * blocks * span : (rb_at + 1) * blocks * span
            ].reshape(blocks, span, channels)


def finish_chunk(chunk, back, mbconv, previous, shape, span, stride_rows, stride_cols):
    rows, cols, channels = shape
    blocks = cols // stride_cols
    row_blocks = rows // stride_rows
    operands = [back, mbconv] + ([] if previous is None else [previous])
    specs = [
        pl.BlockSpec(back.shape, lambda i: (0, 0, 0)),
        pl.BlockSpec(mbconv.shape, lambda i: (0, 0)),
    ] + ([] if previous is None else [pl.BlockSpec(memory_space=pl.ANY)])
    return pl.pallas_call(
        functools.partial(
            finish_kernel, span=span, stride_rows=stride_rows, row_blocks=row_blocks, blocks=blocks
        ),
        grid=(1,),
        in_specs=specs,
        out_specs=pl.BlockSpec((rows, blocks, span, channels), lambda i: (0, 0, chunk, 0)),
        out_shape=jax.ShapeDtypeStruct((rows, blocks, stride_cols, channels), jnp.bfloat16),
        input_output_aliases={} if previous is None else {2: 0},
        cost_estimate=pl.CostEstimate(
            flops=2 * rows * span * blocks * channels * span * row_blocks * blocks,
            bytes_accessed=2 << 20,
            transcendentals=0,
        ),
        name=f"finish_{chunk}",
    )(*operands)


def chunked(
    tokens, expand_weight, depth_kernel, project_weight, norm_gain, attend_weight, output_weight
):
    rows, cols, channels = tokens.shape
    row_count = lax.axis_size("row")
    col_count = lax.axis_size("col")
    devices = row_count * col_count
    stride_rows = rows * row_count // GRID
    stride_cols = cols * col_count // GRID
    blocks = cols // stride_cols
    row_blocks = rows // stride_rows
    span = stride_cols // CHUNKS
    per = row_blocks * blocks
    both = ("row", "col")

    col = lax.axis_index("col")
    edge = jnp.where(col == 0, tokens[:, cols - 1], tokens[:, 0])
    ups = [(r, r + 1) for r in range(row_count - 1)]
    downs = [(r + 1, r) for r in range(row_count - 1)]
    across = lambda pairs: [
        (f * col_count + c, t * col_count + 1 - c) for f, t in pairs for c in range(col_count)
    ]
    up = lax.ppermute(tokens[rows - 1 :], "row", ups)
    down = lax.ppermute(tokens[:1], "row", downs)
    side = lax.ppermute(edge, "col", [(0, 1), (1, 0)])
    side_up = lax.ppermute(edge[rows - 1 :], both, across(ups))
    side_down = lax.ppermute(edge[:1], both, across(downs))
    halos = (up, down, side, side_up, side_down)
    weights = (
        expand_weight,
        depth_kernel.reshape(9, -1),
        project_weight,
        norm_gain.reshape(1, -1),
    )
    col_scalar = col.astype(jnp.int32).reshape(1)

    pieces, keeps = [], []
    for chunk in range(CHUNKS):
        normed, mbconv = mbconv_chunk(
            chunk, span, stride_rows, stride_cols, col_scalar, tokens, halos, weights
        )
        keeps.append(mbconv)
        pieces.append(
            lax.all_to_all(
                normed.reshape(devices, -1, channels), both, split_axis=0, concat_axis=0, tiled=True
            )
        )
    backs = []
    for chunk in range(CHUNKS):
        result = attend_chunk(chunk, pieces[chunk], per, attend_weight, output_weight)
        backs.append(lax.all_to_all(result, both, split_axis=0, concat_axis=0, tiled=True))
    out = None
    for chunk in range(CHUNKS):
        out = finish_chunk(
            chunk, backs[chunk], keeps[chunk], out, tokens.shape, span, stride_rows, stride_cols
        )
    return out.reshape(rows, cols, channels)


def fits(tokens_shape, row_count, col_count):
    rows, cols, channels = tokens_shape
    stride_rows = rows * row_count // GRID
    stride_cols = cols * col_count // GRID
    groups = stride_rows * stride_cols
    return (
        col_count == 2
        and rows % stride_rows == 0
        and cols % stride_cols == 0
        and cols // stride_cols == SUBLANES
        and rows // stride_rows == 2
        and groups % (CHUNKS * row_count * col_count) == 0
        and channels % LANES == 0
    )


def local(
    tokens, expand_weight, depth_kernel, project_weight, norm_gain, attend_weight, output_weight
):
    if fits(tokens.shape, lax.axis_size("row"), lax.axis_size("col")):
        return chunked(
            tokens,
            expand_weight,
            depth_kernel,
            project_weight,
            norm_gain,
            attend_weight,
            output_weight,
        )
    tile_rows, tile_cols, channels = tokens.shape
    padded_in = extended(tokens, (("row", 0), ("col", 1)), 1)
    expanded = expand_tile(padded_in, expand_weight)
    total = jnp.zeros((tile_rows, tile_cols, expanded.shape[2]), jnp.float32)
    for shift_row in range(3):
        for shift_col in range(3):
            total = (
                total
                + expanded[
                    shift_row : shift_row + tile_rows, shift_col : shift_col + tile_cols
                ].astype(jnp.float32)
                * depth_kernel[shift_row, shift_col]
            )
    depth = gelu_tanh(total).astype(jnp.bfloat16)
    branch = jnp.dot(
        depth.reshape(tile_rows * tile_cols, -1), project_weight, preferred_element_type=jnp.float32
    )
    mbconv = (tokens.astype(jnp.float32) + branch.reshape(tile_rows, tile_cols, channels)).astype(
        jnp.bfloat16
    )
    normed = layer_norm(mbconv, norm_gain)
    row_count = lax.axis_size("row")
    col_count = lax.axis_size("col")
    devices = row_count * col_count
    stride_rows = tile_rows * row_count // GRID
    stride_cols = tile_cols * col_count // GRID
    col_blocks = tile_cols // stride_cols
    if row_count % GRID == 0:
        spread_count = stride_rows // tile_rows
        per_dest = tile_rows * stride_cols // devices
        ordered = normed.reshape(tile_rows, col_blocks, stride_cols, channels).transpose(0, 2, 1, 3)
        ordered = ordered.reshape(devices, per_dest, col_blocks, channels)
    else:
        spread_count = 1
        row_blocks = tile_rows // stride_rows
        ordered = normed.reshape(
            row_blocks, stride_rows, col_blocks, stride_cols, channels
        ).transpose(1, 3, 0, 2, 4)
        ordered = ordered.reshape(devices, -1, row_blocks * col_blocks, channels)
    piece = lax.all_to_all(ordered, ("row", "col"), split_axis=0, concat_axis=0, tiled=True)
    items = piece.shape[1]
    per_source = piece.shape[2]
    grouped = piece.reshape(
        row_count // spread_count, spread_count, col_count, items, per_source, channels
    )
    grouped = grouped.transpose(3, 1, 0, 2, 4, 5).reshape(items * spread_count, -1, channels)
    result = attend_groups(grouped, attend_weight, output_weight)
    result = result.reshape(
        items, spread_count, row_count // spread_count, col_count, per_source, channels
    )
    returned = lax.all_to_all(
        result.transpose(2, 1, 3, 0, 4, 5).reshape(devices, items, per_source, channels),
        ("row", "col"),
        split_axis=0,
        concat_axis=0,
        tiled=True,
    )
    if row_count % GRID == 0:
        attention = returned.reshape(tile_rows, stride_cols, col_blocks, channels).transpose(
            0, 2, 1, 3
        )
    else:
        row_blocks = tile_rows // stride_rows
        attention = returned.reshape(
            stride_rows, stride_cols, row_blocks, col_blocks, channels
        ).transpose(2, 0, 3, 1, 4)
    attention = attention.reshape(tile_rows, tile_cols, channels)
    return (mbconv.astype(jnp.float32) + attention.astype(jnp.float32)).astype(jnp.bfloat16)


def solution(mesh):
    placed = (P(("parts", "row"), "col", None), P(), P(), P(), P(), P(), P())
    return jax.shard_map(
        local,
        mesh=mesh,
        in_specs=placed,
        out_specs=P(("parts", "row"), "col", None),
        check_vma=False,
    )
```

```python
import functools
import math

import jax
import jax.numpy as jnp
from jax import lax
from jax.experimental import pallas as pl
from jax.experimental.pallas import tpu as pltpu
from jax.sharding import PartitionSpec as P

HEADS = 16
HEAD_DIM = 32
GRID = 16
CHUNKS = 2
SUBLANES = 8
LANES = 128
LOG2E = 1.4426950408889634
BLOCK = 256
GELU_ONE = math.sqrt(2 / math.pi)
GELU_THREE = 0.044715 * GELU_ONE
TAP_SCALE = 0.5 * math.sqrt(GELU_THREE)
BRANCH_SCALE = 0.5 / math.sqrt(GELU_THREE)


def extended(cells, sides, width):
    for axis, dim in sides:
        count = lax.axis_size(axis)
        ends = count - 1
        head = lax.slice_in_dim(cells, 0, width, axis=dim)
        tail = lax.slice_in_dim(cells, cells.shape[dim] - width, cells.shape[dim], axis=dim)
        cells = jnp.concatenate(
            [
                lax.ppermute(tail, axis, [(i, (i + 1) % count) for i in range(ends)]),
                cells,
                lax.ppermute(head, axis, [((i + 1) % count, i) for i in range(ends)]),
            ],
            axis=dim,
        )
    return cells


def gelu_tanh(values):
    return jax.nn.gelu(values, approximate=True)


def gelu_twice(v):
    return v + v * jnp.tanh(v * (GELU_ONE + GELU_THREE * (v * v)))


def gelu_scaled(w):
    return w + w * jnp.tanh(w * (GELU_ONE / math.sqrt(GELU_THREE) + w * w))


def expand_tile(inputs, expand_weight):
    shape = inputs.shape
    product = jnp.dot(
        inputs.reshape(-1, shape[2]), expand_weight, preferred_element_type=jnp.float32
    )
    return gelu_tanh(product).astype(jnp.bfloat16).reshape(shape[0], shape[1], -1)


def layer_norm(values, gain):
    values = values.astype(jnp.float32)
    center = jnp.mean(values, axis=-1, keepdims=True)
    spread = jnp.mean((values - center) ** 2, axis=-1, keepdims=True)
    return ((values - center) * lax.rsqrt(spread + 1e-05) * gain).astype(jnp.bfloat16)


def attend_groups(groups, attend_weight, output_weight):
    count, members, channels = groups.shape
    projected = jnp.dot(
        groups.reshape(count * members, channels), attend_weight, preferred_element_type=jnp.float32
    )
    projected = projected.astype(jnp.bfloat16).reshape(count, members, 3, HEADS, HEAD_DIM)
    query_heads = projected[:, :, 0]
    key_heads = projected[:, :, 1]
    value_heads = projected[:, :, 2]
    scores = jnp.einsum(
        "nqhd,nkhd->nhqk", query_heads, key_heads, preferred_element_type=jnp.float32
    ) / math.sqrt(HEAD_DIM)
    soft = jax.nn.softmax(scores, axis=-1).astype(jnp.bfloat16)
    heads_out = jnp.einsum("nhqk,nkhd->nqhd", soft, value_heads, preferred_element_type=jnp.float32)
    heads_out = heads_out.astype(jnp.bfloat16).reshape(count * members, channels)
    result = jnp.dot(heads_out, output_weight, preferred_element_type=jnp.float32).astype(
        jnp.bfloat16
    )
    return result.reshape(count, members, channels)


def expand_kernel(
    col_ref, x_ref, side_ref, expand_ref, ordered_ref, *rest, stride_cols, span, chunks
):
    expanded_refs = rest
    step = pl.program_id(0)
    rows, cols, channels = x_ref.shape
    blocks = cols // stride_cols
    size = (stride_cols + 2) * blocks
    part = (span + 2) * blocks

    @pl.when(step == 0)
    def _():
        for row in range(rows):
            ordered_ref[row] = arrange(
                x_ref[row], side_ref[row : row + 1, :], col_ref[0] == 0, -1, size, stride_cols, blocks,
                True, True,
            )

    for half in range(2):
        for row in range(rows):
            product = jnp.dot(
                ordered_ref[row],
                expand_ref[:, half * BLOCK : (half + 1) * BLOCK],
                preferred_element_type=jnp.float32,
            )
            value = gelu_twice(product).astype(jnp.bfloat16)
            for chunk in range(chunks):
                begin = chunk * span * blocks
                expanded_refs[chunk][half, row] = value[begin : begin + part]


def arrange(source, edge, is_left, start, size, stride_cols, blocks, first, last):
    cols, channels = source.shape
    at = lax.broadcasted_iota(jnp.int32, (size, cols), 0)
    want = (at % blocks) * stride_cols + at // blocks + start
    select = (lax.broadcasted_iota(jnp.int32, (size, cols), 1) == want).astype(jnp.bfloat16)
    picked = jnp.dot(select, source, preferred_element_type=jnp.float32)
    position = lax.broadcasted_iota(jnp.int32, (size, channels), 0)
    edge = edge.astype(jnp.float32)
    zero = jnp.zeros_like(edge)
    if first:
        picked = jnp.where(position == 0, jnp.where(is_left, zero, edge), picked)
    if last:
        picked = jnp.where(position == size - 1, jnp.where(is_left, edge, zero), picked)
    return picked.astype(jnp.bfloat16)


def expand_rows(col, tokens, side, expand_weight, stride_cols, span):
    rows, cols, channels = tokens.shape
    hidden = expand_weight.shape[1]
    blocks = cols // stride_cols
    size = (stride_cols + 2) * blocks
    part = (span + 2) * blocks
    steps = hidden // BLOCK
    return pl.pallas_call(
        functools.partial(expand_kernel, stride_cols=stride_cols, span=span, chunks=CHUNKS),
        grid_spec=pltpu.PrefetchScalarGridSpec(
            num_scalar_prefetch=1,
            grid=(steps // 2,),
            in_specs=[
                pl.BlockSpec(tokens.shape, lambda i, c: (0, 0, 0)),
                pl.BlockSpec(side.shape, lambda i, c: (0, 0)),
                pl.BlockSpec((channels, 2 * BLOCK), lambda i, c: (0, i)),
            ],
            out_specs=[pl.BlockSpec((rows, size, channels), lambda i, c: (0, 0, 0))]
            + [pl.BlockSpec((2, rows, part, BLOCK), lambda i, c: (i, 0, 0, 0))] * CHUNKS,
        ),
        out_shape=[jax.ShapeDtypeStruct((rows, size, channels), jnp.bfloat16)]
        + [jax.ShapeDtypeStruct((steps, rows, part, BLOCK), jnp.bfloat16)] * CHUNKS,
        compiler_params=pltpu.CompilerParams(dimension_semantics=("arbitrary",)),
        cost_estimate=pl.CostEstimate(
            flops=2 * rows * size * channels * hidden, bytes_accessed=8 << 20, transcendentals=0
        ),
        name="expand",
    )(col, tokens, side, expand_weight)


def mbconv_kernel(
    col_ref, up_ref, down_ref, side_up_ref, side_down_ref, ordered_ref, own_ref,
    expand_ref, taps_ref, project_old_ref, project_new_ref, project_last_ref, gain_ref,
    normed_ref, mbconv_ref,
    halo, edge_rows, depth_a, depth_b, acc,
    *, chunk, span, stride_cols, stride_rows, rows,
):
    step = pl.program_id(0)
    channels = up_ref.shape[2]
    blocks = up_ref.shape[1] // stride_cols
    wide = span + 2
    size = wide * blocks
    row_blocks = rows // stride_rows
    members = row_blocks * blocks

    @pl.when(step == 0)
    def _():
        for side, (source_ref, edge_ref) in enumerate(
            ((up_ref, side_up_ref), (down_ref, side_down_ref))
        ):
            halo[side] = arrange(
                source_ref[0], edge_ref[...], col_ref[0] == 0, chunk * span - 1, size, stride_cols,
                blocks, chunk * span == 0, (chunk + 1) * span == stride_cols,
            )
        depth_b[...] = jnp.zeros_like(depth_b)
        acc[...] = jnp.zeros_like(acc)

    for half, depth in ((0, depth_a), (1, depth_b)):
        lanes = slice(half * BLOCK, (half + 1) * BLOCK)
        for side in range(2):
            product = jnp.dot(halo[side], expand_ref[:, lanes], preferred_element_type=jnp.float32)
            edge_rows[half, side] = gelu_twice(product).reshape(wide, blocks, BLOCK)
        if half == 0:
            acc[...] = acc[...] + jnp.dot(
                depth_b[...], project_old_ref[...], preferred_element_type=jnp.float32
            )
        for lane in range(0, BLOCK, LANES):
            taps = [
                [
                    taps_ref[dr, dc : dc + 1, half * BLOCK + lane : half * BLOCK + lane + LANES]
                    * TAP_SCALE
                    for dc in range(3)
                ]
                for dr in range(3)
            ]
            for pair in range(0, span, 2):
                source = []
                for row in range(rows + 2):
                    if row == 0 or row == rows + 1:
                        source.append(
                            [
                                edge_rows[half, min(row, 1), pair + k, :, lane : lane + LANES]
                                for k in range(4)
                            ]
                        )
                    else:
                        source.append(
                            [
                                own_ref[
                                    half, row - 1, (pair + k) * blocks : (pair + k + 2) * blocks,
                                    lane : lane + LANES,
                                ].astype(jnp.float32)[j * blocks : (j + 1) * blocks]
                                for k in (0, 2)
                                for j in (0, 1)
                            ]
                        )
                for b in (0, 1):
                    for hm in range(stride_rows):
                        parts = []
                        for rb in range(row_blocks):
                            row = rb * stride_rows + hm
                            total = None
                            for dr in range(3):
                                for dc in range(3):
                                    term = source[row + dr][b + dc] * taps[dr][dc]
                                    total = term if total is None else total + term
                            parts.append(gelu_scaled(total))
                        place = (hm * span + pair + b) * members
                        depth[place : place + members, lane : lane + LANES] = jnp.concatenate(
                            parts, axis=0
                        ).astype(jnp.bfloat16)
        if half == 0:
            acc[...] = acc[...] + jnp.dot(
                depth_a[...], project_new_ref[...], preferred_element_type=jnp.float32
            )

    @pl.when(step == pl.num_programs(0) - 1)
    def _():
        gain = gain_ref[...]
        acc[...] = acc[...] + jnp.dot(
            depth_b[...], project_last_ref[...], preferred_element_type=jnp.float32
        )
        for hm in range(stride_rows):
            for b in range(span):
                pieces = []
                for rb in range(row_blocks):
                    begin = (chunk * span + b + 1) * blocks
                    low = begin - begin % 16
                    pair = ordered_ref[rb * stride_rows + hm, low : low + 16, :].astype(jnp.float32)
                    pieces.append(pair[begin - low : begin - low + blocks])
                place = (hm * span + b) * members
                branch = acc[place : place + members, :]
                mixed = jnp.concatenate(pieces, axis=0) + branch * BRANCH_SCALE
                mixed = mixed.astype(jnp.bfloat16)
                mbconv_ref[place : place + members, :] = mixed
                mixed = mixed.astype(jnp.float32)
                center = jnp.mean(mixed, axis=-1, keepdims=True)
                moved = mixed - center
                spread = jnp.mean(moved * moved, axis=-1, keepdims=True)
                normed_ref[place : place + members, :] = (
                    moved * lax.rsqrt(spread + 1e-05) * gain
                ).astype(jnp.bfloat16)


def mbconv_chunk(chunk, span, stride_rows, stride_cols, col, halos, ordered, own, weights):
    rows = own.shape[1]
    cols, channels = halos[0].shape[1:]
    expand_weight, taps, project_weight, gain = weights
    hidden = expand_weight.shape[1]
    blocks = cols // stride_cols
    count = rows * span * blocks
    size = (span + 2) * blocks
    last = hidden // BLOCK - 1

    def whole(array):
        return pl.BlockSpec(array.shape, lambda i, c: (0,) * array.ndim)

    grid_spec = pltpu.PrefetchScalarGridSpec(
        num_scalar_prefetch=1,
        grid=(hidden // (2 * BLOCK),),
        in_specs=[whole(h) for h in halos]
        + [
            whole(ordered),
            pl.BlockSpec((2, rows, size, BLOCK), lambda i, c: (i, 0, 0, 0)),
            pl.BlockSpec((channels, 2 * BLOCK), lambda i, c: (0, i)),
            pl.BlockSpec((3, 3, 2 * BLOCK), lambda i, c: (0, 0, i)),
            pl.BlockSpec((BLOCK, channels), lambda i, c: (jnp.maximum(2 * i - 1, 0), 0)),
            pl.BlockSpec((BLOCK, channels), lambda i, c: (2 * i, 0)),
            pl.BlockSpec((BLOCK, channels), lambda i, c: (last, 0)),
            whole(gain),
        ],
        out_specs=[pl.BlockSpec((count, channels), lambda i, c: (0, 0))] * 2,
        scratch_shapes=[
            pltpu.VMEM((2, size, channels), jnp.bfloat16),
            pltpu.VMEM((2, 2, span + 2, blocks, BLOCK), jnp.float32),
            pltpu.VMEM((count, BLOCK), jnp.bfloat16),
            pltpu.VMEM((count, BLOCK), jnp.bfloat16),
            pltpu.VMEM((count, channels), jnp.float32),
        ],
    )
    return pl.pallas_call(
        functools.partial(
            mbconv_kernel, chunk=chunk, span=span, stride_cols=stride_cols, stride_rows=stride_rows,
            rows=rows,
        ),
        grid_spec=grid_spec,
        out_shape=[jax.ShapeDtypeStruct((count, channels), jnp.bfloat16)] * 2,
        compiler_params=pltpu.CompilerParams(dimension_semantics=("arbitrary",)),
        cost_estimate=pl.CostEstimate(
            flops=4 * count * channels * hidden, bytes_accessed=8 << 20, transcendentals=0
        ),
        name=f"mbconv_{chunk}",
    )(
        col, *halos, ordered, own, expand_weight, taps, project_weight, project_weight,
        project_weight, gain,
    )


def attend_kernel(x_ref, attend_ref, output_ref, out_ref):
    sources, per, channels = x_ref.shape
    members = sources * per
    x = x_ref[...].reshape(members, channels)
    scale = LOG2E / math.sqrt(HEAD_DIM)
    fold = LANES // HEAD_DIM
    lane = lax.broadcasted_iota(jnp.int32, (members, LANES), 1) // HEAD_DIM
    ones = jnp.ones((members, LANES), jnp.bfloat16)
    tiles = []
    projected = [
        jnp.dot(
            x, attend_ref[:, begin : begin + BLOCK], preferred_element_type=jnp.float32
        )
        for begin in range(0, 3 * channels, BLOCK)
    ]

    def cut(begin):
        return projected[begin // BLOCK][:, begin % BLOCK : begin % BLOCK + LANES]

    for tile in range(channels // LANES):
        begin = tile * LANES
        query = (cut(begin) * scale).astype(jnp.bfloat16)
        key = cut(channels + begin).astype(jnp.bfloat16)
        value = cut(2 * channels + begin).astype(jnp.bfloat16)
        upper = None
        for head in range(fold):
            inside = lane == head
            key_head = jnp.where(inside, key, jnp.zeros_like(key))
            value_head = jnp.where(inside, value, jnp.zeros_like(value))
            scores = lax.dot_general(
                query, key_head, (((1,), (1,)), ((), ())), preferred_element_type=jnp.float32
            )
            top = jnp.max(scores, axis=-1, keepdims=True)
            weight = jnp.exp2(scores - top).astype(jnp.bfloat16)
            mixed = jnp.dot(
                weight,
                jnp.concatenate([value_head, ones], axis=1),
                preferred_element_type=jnp.float32,
            )
            if upper is None:
                upper, lower = mixed[:, :LANES], mixed[:, LANES:]
            else:
                upper = upper + mixed[:, :LANES]
                lower = jnp.where(inside, mixed[:, LANES:], lower)
        tiles.append((upper / lower).astype(jnp.bfloat16))
    heads_out = jnp.concatenate(tiles, axis=1)
    result = jnp.dot(heads_out, output_ref[...], preferred_element_type=jnp.float32)
    out_ref[...] = result.astype(jnp.bfloat16).reshape(sources, per, channels)


def attend_chunk(chunk, piece, per, attend_weight, output_weight):
    sources, length, channels = piece.shape
    items = length // per
    members = sources * per
    spec = pl.BlockSpec((sources, per, channels), lambda i: (0, i, 0))
    return pl.pallas_call(
        attend_kernel,
        grid=(items,),
        in_specs=[
            spec,
            pl.BlockSpec(attend_weight.shape, lambda i: (0, 0)),
            pl.BlockSpec(output_weight.shape, lambda i: (0, 0)),
        ],
        out_specs=spec,
        out_shape=jax.ShapeDtypeStruct(piece.shape, jnp.bfloat16),
        compiler_params=pltpu.CompilerParams(dimension_semantics=("arbitrary",)),
        cost_estimate=pl.CostEstimate(
            flops=items * members * channels * (8 * channels + 8 * members),
            bytes_accessed=4 << 20,
            transcendentals=0,
        ),
        name=f"attend_{chunk}",
    )(piece, attend_weight, output_weight)


def finish_kernel(*refs, span, stride_rows, row_blocks, blocks):
    back_ref, mbconv_ref, out_ref = refs[0], refs[1], refs[-1]
    channels = back_ref.shape[-1]
    length = span * row_blocks * blocks
    total = back_ref[...].reshape(-1, channels).astype(jnp.float32) + mbconv_ref[...].astype(
        jnp.float32
    )
    total = total.astype(jnp.bfloat16)
    at = lax.broadcasted_iota(jnp.int32, (length, length), 0)
    b = at % span
    a = (at // span) % blocks
    rb = at // (span * blocks)
    select = lax.broadcasted_iota(jnp.int32, (length, length), 1) == (b * row_blocks + rb) * blocks + a
    select = select.astype(jnp.bfloat16)
    for hm in range(stride_rows):
        placed = jnp.dot(
            select, total[hm * length : (hm + 1) * length], preferred_element_type=jnp.float32
        ).astype(jnp.bfloat16)
        for rb_at in range(row_blocks):
            out_ref[rb_at * stride_rows + hm] = placed[
                rb_at * blocks * span : (rb_at + 1) * blocks * span
            ].reshape(blocks, span, channels)


def finish_chunk(chunk, back, mbconv, previous, shape, span, stride_rows, stride_cols):
    rows, cols, channels = shape
    blocks = cols // stride_cols
    row_blocks = rows // stride_rows
    operands = [back, mbconv] + ([] if previous is None else [previous])
    specs = [
        pl.BlockSpec(back.shape, lambda i: (0, 0, 0)),
        pl.BlockSpec(mbconv.shape, lambda i: (0, 0)),
    ] + ([] if previous is None else [pl.BlockSpec(memory_space=pl.ANY)])
    return pl.pallas_call(
        functools.partial(
            finish_kernel, span=span, stride_rows=stride_rows, row_blocks=row_blocks, blocks=blocks
        ),
        grid=(1,),
        in_specs=specs,
        out_specs=pl.BlockSpec((rows, blocks, span, channels), lambda i: (0, 0, chunk, 0)),
        out_shape=jax.ShapeDtypeStruct((rows, blocks, stride_cols, channels), jnp.bfloat16),
        input_output_aliases={} if previous is None else {2: 0},
        cost_estimate=pl.CostEstimate(
            flops=2 * rows * span * blocks * channels * span * row_blocks * blocks,
            bytes_accessed=2 << 20,
            transcendentals=0,
        ),
        name=f"finish_{chunk}",
    )(*operands)


def chunked(
    tokens, expand_weight, depth_kernel, project_weight, norm_gain, attend_weight, output_weight
):
    rows, cols, channels = tokens.shape
    row_count = lax.axis_size("row")
    col_count = lax.axis_size("col")
    devices = row_count * col_count
    stride_rows = rows * row_count // GRID
    stride_cols = cols * col_count // GRID
    blocks = cols // stride_cols
    row_blocks = rows // stride_rows
    span = stride_cols // CHUNKS
    per = row_blocks * blocks
    both = ("row", "col")

    col = lax.axis_index("col")
    edge = jnp.where(col == 0, tokens[:, cols - 1], tokens[:, 0])
    ups = [(r, r + 1) for r in range(row_count - 1)]
    downs = [(r + 1, r) for r in range(row_count - 1)]
    across = lambda pairs: [
        (f * col_count + c, t * col_count + 1 - c) for f, t in pairs for c in range(col_count)
    ]
    side = lax.ppermute(edge, "col", [(0, 1), (1, 0)])
    side_up = lax.ppermute(edge[rows - 1 :], both, across(ups))
    side_down = lax.ppermute(edge[:1], both, across(downs))
    up = lax.ppermute(tokens[rows - 1 :], "row", ups)
    down = lax.ppermute(tokens[:1], "row", downs)
    halos = (up, down, side_up, side_down)
    weights = (expand_weight, depth_kernel, project_weight, norm_gain.reshape(1, -1))
    col_scalar = col.astype(jnp.int32).reshape(1)
    ordered, *own = expand_rows(col_scalar, tokens, side, expand_weight, stride_cols, span)

    pieces, keeps = [], []
    for chunk in range(CHUNKS):
        normed, mbconv = mbconv_chunk(
            chunk, span, stride_rows, stride_cols, col_scalar, halos, ordered, own[chunk], weights
        )
        keeps.append(mbconv)
        pieces.append(
            lax.all_to_all(
                normed.reshape(devices, -1, channels), both, split_axis=0, concat_axis=0, tiled=True
            )
        )
    backs = []
    for chunk in range(CHUNKS):
        result = attend_chunk(chunk, pieces[chunk], per, attend_weight, output_weight)
        backs.append(lax.all_to_all(result, both, split_axis=0, concat_axis=0, tiled=True))
    out = None
    for chunk in range(CHUNKS):
        out = finish_chunk(
            chunk, backs[chunk], keeps[chunk], out, tokens.shape, span, stride_rows, stride_cols
        )
    return out.reshape(rows, cols, channels)


def fits(tokens_shape, hidden, row_count, col_count):
    rows, cols, channels = tokens_shape
    stride_rows = rows * row_count // GRID
    stride_cols = cols * col_count // GRID
    groups = stride_rows * stride_cols
    return (
        col_count == 2
        and rows % stride_rows == 0
        and cols % stride_cols == 0
        and cols // stride_cols == SUBLANES
        and rows // stride_rows == 2
        and groups % (CHUNKS * row_count * col_count) == 0
        and channels % BLOCK == 0
        and hidden % (2 * BLOCK) == 0
        and stride_cols // CHUNKS % 2 == 0
    )


def local(
    tokens, expand_weight, depth_kernel, project_weight, norm_gain, attend_weight, output_weight
):
    if fits(tokens.shape, expand_weight.shape[1], lax.axis_size("row"), lax.axis_size("col")):
        return chunked(
            tokens,
            expand_weight,
            depth_kernel,
            project_weight,
            norm_gain,
            attend_weight,
            output_weight,
        )
    tile_rows, tile_cols, channels = tokens.shape
    padded_in = extended(tokens, (("row", 0), ("col", 1)), 1)
    expanded = expand_tile(padded_in, expand_weight)
    total = jnp.zeros((tile_rows, tile_cols, expanded.shape[2]), jnp.float32)
    for shift_row in range(3):
        for shift_col in range(3):
            total = (
                total
                + expanded[
                    shift_row : shift_row + tile_rows, shift_col : shift_col + tile_cols
                ].astype(jnp.float32)
                * depth_kernel[shift_row, shift_col]
            )
    depth = gelu_tanh(total).astype(jnp.bfloat16)
    branch = jnp.dot(
        depth.reshape(tile_rows * tile_cols, -1), project_weight, preferred_element_type=jnp.float32
    )
    mbconv = (tokens.astype(jnp.float32) + branch.reshape(tile_rows, tile_cols, channels)).astype(
        jnp.bfloat16
    )
    normed = layer_norm(mbconv, norm_gain)
    row_count = lax.axis_size("row")
    col_count = lax.axis_size("col")
    devices = row_count * col_count
    stride_rows = tile_rows * row_count // GRID
    stride_cols = tile_cols * col_count // GRID
    col_blocks = tile_cols // stride_cols
    if row_count % GRID == 0:
        spread_count = stride_rows // tile_rows
        per_dest = tile_rows * stride_cols // devices
        ordered = normed.reshape(tile_rows, col_blocks, stride_cols, channels).transpose(0, 2, 1, 3)
        ordered = ordered.reshape(devices, per_dest, col_blocks, channels)
    else:
        spread_count = 1
        row_blocks = tile_rows // stride_rows
        ordered = normed.reshape(
            row_blocks, stride_rows, col_blocks, stride_cols, channels
        ).transpose(1, 3, 0, 2, 4)
        ordered = ordered.reshape(devices, -1, row_blocks * col_blocks, channels)
    piece = lax.all_to_all(ordered, ("row", "col"), split_axis=0, concat_axis=0, tiled=True)
    items = piece.shape[1]
    per_source = piece.shape[2]
    grouped = piece.reshape(
        row_count // spread_count, spread_count, col_count, items, per_source, channels
    )
    grouped = grouped.transpose(3, 1, 0, 2, 4, 5).reshape(items * spread_count, -1, channels)
    result = attend_groups(grouped, attend_weight, output_weight)
    result = result.reshape(
        items, spread_count, row_count // spread_count, col_count, per_source, channels
    )
    returned = lax.all_to_all(
        result.transpose(2, 1, 3, 0, 4, 5).reshape(devices, items, per_source, channels),
        ("row", "col"),
        split_axis=0,
        concat_axis=0,
        tiled=True,
    )
    if row_count % GRID == 0:
        attention = returned.reshape(tile_rows, stride_cols, col_blocks, channels).transpose(
            0, 2, 1, 3
        )
    else:
        row_blocks = tile_rows // stride_rows
        attention = returned.reshape(
            stride_rows, stride_cols, row_blocks, col_blocks, channels
        ).transpose(2, 0, 3, 1, 4)
    attention = attention.reshape(tile_rows, tile_cols, channels)
    return (mbconv.astype(jnp.float32) + attention.astype(jnp.float32)).astype(jnp.bfloat16)


def solution(mesh):
    placed = (P(("parts", "row"), "col", None), P(), P(), P(), P(), P(), P())
    return jax.shard_map(
        local,
        mesh=mesh,
        in_specs=placed,
        out_specs=P(("parts", "row"), "col", None),
        check_vma=False,
    )
```

```python
import functools
import math

import jax
import jax.numpy as jnp
from jax import lax
from jax.experimental import pallas as pl
from jax.experimental.pallas import tpu as pltpu
from jax.sharding import PartitionSpec as P


HEADS = 16
HEAD_DIM = 32
GRID = 16
HALVES = 2
SUBLANES = 8
LANES = 128
LOG2E = 1.4426950408889634
BLOCK = 256
GELU_ONE = math.sqrt(2 / math.pi)
GELU_THREE = 0.044715 * GELU_ONE
CUBE_ROOT = GELU_THREE ** (1 / 3)
TAP_SCALE = 0.5 * CUBE_ROOT
BRANCH_SCALE = 0.5 / CUBE_ROOT


def extended(cells, sides, width):
    for axis, dim in sides:
        count = lax.axis_size(axis)
        ends = count - 1
        head = lax.slice_in_dim(cells, 0, width, axis=dim)
        tail = lax.slice_in_dim(cells, cells.shape[dim] - width, cells.shape[dim], axis=dim)
        cells = jnp.concatenate(
            [
                lax.ppermute(tail, axis, [(i, (i + 1) % count) for i in range(ends)]),
                cells,
                lax.ppermute(head, axis, [((i + 1) % count, i) for i in range(ends)]),
            ],
            axis=dim,
        )
    return cells


def gelu_tanh(values):
    return jax.nn.gelu(values, approximate=True)


def gelu_twice(v):
    return v + v * jnp.tanh(v * (GELU_ONE + GELU_THREE * (v * v)))


def gelu_scaled(w):
    return w + w * jnp.tanh(w * (GELU_ONE / CUBE_ROOT + w * w))


def expand_tile(inputs, expand_weight):
    shape = inputs.shape
    product = jnp.dot(
        inputs.reshape(-1, shape[2]), expand_weight, preferred_element_type=jnp.float32
    )
    return gelu_tanh(product).astype(jnp.bfloat16).reshape(shape[0], shape[1], -1)


def layer_norm(values, gain):
    values = values.astype(jnp.float32)
    center = jnp.mean(values, axis=-1, keepdims=True)
    spread = jnp.mean((values - center) ** 2, axis=-1, keepdims=True)
    return ((values - center) * lax.rsqrt(spread + 1e-05) * gain).astype(jnp.bfloat16)


def attend_groups(groups, attend_weight, output_weight):
    count, members, channels = groups.shape
    projected = jnp.dot(
        groups.reshape(count * members, channels), attend_weight, preferred_element_type=jnp.float32
    )
    projected = projected.astype(jnp.bfloat16).reshape(count, members, 3, HEADS, HEAD_DIM)
    query_heads = projected[:, :, 0]
    key_heads = projected[:, :, 1]
    value_heads = projected[:, :, 2]
    scores = jnp.einsum(
        "nqhd,nkhd->nhqk", query_heads, key_heads, preferred_element_type=jnp.float32
    ) / math.sqrt(HEAD_DIM)
    soft = jax.nn.softmax(scores, axis=-1).astype(jnp.bfloat16)
    heads_out = jnp.einsum("nhqk,nkhd->nqhd", soft, value_heads, preferred_element_type=jnp.float32)
    heads_out = heads_out.astype(jnp.bfloat16).reshape(count * members, channels)
    result = jnp.dot(heads_out, output_weight, preferred_element_type=jnp.float32).astype(
        jnp.bfloat16
    )
    return result.reshape(count, members, channels)


def arrange_kernel(place_ref, *refs, stride_cols, share):
    count = len(refs) // 3
    cols, _ = refs[0].shape[1:]
    size = refs[-1].shape[1]
    col = place_ref[0]
    at = lax.broadcasted_iota(jnp.int32, (size, cols), 0)
    want = (at % GRID) * stride_cols + at // GRID + (col * share - 1)
    index = lax.broadcasted_iota(jnp.int32, (size, cols), 1)
    select_own = (index + col * cols == want).astype(jnp.bfloat16)
    select_other = (index + (1 - col) * cols == want).astype(jnp.bfloat16)
    for own_ref, other_ref, ordered_ref in zip(refs[:count], refs[count : 2 * count], refs[2 * count :]):
        for row in range(own_ref.shape[0]):
            picked = jnp.dot(select_own, own_ref[row], preferred_element_type=jnp.float32) + jnp.dot(
                select_other, other_ref[row], preferred_element_type=jnp.float32
            )
            ordered_ref[row] = picked.astype(jnp.bfloat16)


VMEM = pl.BlockSpec(memory_space=pltpu.VMEM)
SMEM = pl.BlockSpec(memory_space=pltpu.SMEM)
MIB = 1 << 20


def call(kernel, place, operands, shapes, flops, limit, scratch=(), **options):
    return pl.pallas_call(
        kernel,
        in_specs=[SMEM] + [VMEM] * len(operands),
        out_specs=[VMEM] * len(shapes),
        out_shape=[jax.ShapeDtypeStruct(shape, jnp.bfloat16) for shape in shapes],
        scratch_shapes=list(scratch),
        compiler_params=pltpu.CompilerParams(vmem_limit_bytes=limit),
        cost_estimate=pl.CostEstimate(flops=flops, bytes_accessed=1 << 20, transcendentals=0),
    )(place, *operands)


def arrange(place, owns, others, stride_cols, share):
    cols, channels = owns[0].shape[1:]
    size = (share + 2) * GRID
    return call(
        functools.partial(arrange_kernel, stride_cols=stride_cols, share=share),
        place,
        [*owns, *others],
        [(own.shape[0], size, channels) for own in owns],
        sum(4 * own.shape[0] * size * cols * channels for own in owns),
        8 * MIB,
    )


def expand_kernel(place_ref, ordered_ref, expand_ref, expanded_ref):
    rows = ordered_ref.shape[0]
    hidden = expand_ref.shape[1]

    def step(index, carry):
        for half in range(2):
            lanes = pl.ds(pl.multiple_of(index * 2 * BLOCK + half * BLOCK, BLOCK), BLOCK)
            for row in range(rows):
                product = jnp.dot(
                    ordered_ref[row], expand_ref[:, lanes], preferred_element_type=jnp.float32
                )
                expanded_ref[2 * index + half, row] = gelu_twice(product).astype(jnp.bfloat16)
        return carry

    lax.fori_loop(0, hidden // (2 * BLOCK), step, 0)


def expand_rows(place, ordered, expand_weight):
    rows, size, channels = ordered.shape
    hidden = expand_weight.shape[1]
    return call(
        expand_kernel,
        place,
        [ordered, expand_weight],
        [(hidden // BLOCK, rows, size, BLOCK)],
        2 * rows * size * channels * hidden,
        8 * MIB,
    )[0]


def mbconv_kernel(
    place_ref, up_ref, down_ref, ordered_ref, own_ref,
    expand_ref, taps_ref, project_ref, gain_ref,
    mbconv_ref, *rest,
    far, span, stride_rows,
):
    *normed_refs, edge_rows, depth_a, depth_b, acc = rest
    hidden = expand_ref.shape[1]
    rows = ordered_ref.shape[0]
    row_blocks = rows // stride_rows
    owners = len(normed_refs)
    spot_half = place_ref[1] // owners
    half_at = 1 - spot_half if far else spot_half
    begin = pl.multiple_of(half_at * (span * GRID), GRID)
    part = (span + 2) * GRID

    depth_b[...] = jnp.zeros_like(depth_b)
    acc[...] = jnp.zeros_like(acc)

    def step(index, carry):
        for half, depth in ((0, depth_a), (1, depth_b)):
            block = 2 * index + half
            for side, ref in enumerate((up_ref, down_ref)):
                product = jnp.dot(
                    ref[0, pl.ds(begin, part), :],
                    expand_ref[:, pl.ds(block * BLOCK, BLOCK)],
                    preferred_element_type=jnp.float32,
                )
                edge_rows[half, side] = gelu_twice(product)
            if half == 0:
                acc[...] = acc[...] + jnp.dot(
                    depth_b[...],
                    project_ref[pl.ds(jnp.maximum(block - 1, 0) * BLOCK, BLOCK), :],
                    preferred_element_type=jnp.float32,
                )
            for lane in range(0, BLOCK, LANES):
                lanes = slice(lane, lane + LANES)
                taps = [
                    [
                        taps_ref[dr, dc : dc + 1, pl.ds(block * BLOCK + lane, LANES)]
                        * TAP_SCALE
                        for dc in range(3)
                    ]
                    for dr in range(3)
                ]
                for pair in range(0, span, 2):
                    parts = {}
                    for low in range(0, GRID, SUBLANES):
                        source = []
                        for row in range(rows + 2):
                            tiles = []
                            for k in range(4):
                                at = (pair + k) * GRID
                                if row == 0 or row == rows + 1:
                                    at += low
                                    tiles.append(edge_rows[half, min(row, 1), at : at + SUBLANES, lanes])
                                else:
                                    tile = own_ref[block, row - 1, pl.ds(begin + at, GRID), lanes]
                                    tiles.append(tile.astype(jnp.float32)[low : low + SUBLANES])
                            source.append(tiles)
                        for b in (0, 1):
                            for row in range(rows):
                                total = None
                                for dr in range(3):
                                    for dc in range(3):
                                        term = source[row + dr][b + dc] * taps[dr][dc]
                                        total = term if total is None else total + term
                                parts.setdefault((row, b), []).append(gelu_scaled(total))
                    for (row, b), tiles in parts.items():
                        spot = ((row % stride_rows) * span + pair + b) * row_blocks + row // stride_rows
                        depth[spot * GRID : (spot + 1) * GRID, lanes] = jnp.concatenate(
                            tiles, axis=0
                        ).astype(jnp.bfloat16)
            if half == 0:
                acc[...] = acc[...] + jnp.dot(
                    depth_a[...],
                    project_ref[pl.ds(block * BLOCK, BLOCK), :],
                    preferred_element_type=jnp.float32,
                )
        return carry

    lax.fori_loop(0, hidden // (2 * BLOCK), step, 0)

    gain = gain_ref[...]
    acc[...] = acc[...] + jnp.dot(
        depth_b[...],
        project_ref[hidden - BLOCK : hidden, :],
        preferred_element_type=jnp.float32,
    )
    members = row_blocks * GRID
    per_row = stride_rows * span // owners
    for k, normed_ref in enumerate(normed_refs):
        owner = (place_ref[1] % owners) ^ k
        hm = owner // (owners // stride_rows)
        first = (owner % (owners // stride_rows)) * per_row
        for item in range(per_row):
            for rb in range(row_blocks):
                spot = pl.multiple_of((owner * per_row + item) * members + rb * GRID, GRID)
                column = pl.multiple_of(begin + (first + item + 1) * GRID, GRID)
                tokens = ordered_ref[rb * stride_rows + hm, pl.ds(column, GRID), :]
                mixed = tokens.astype(jnp.float32) + acc[pl.ds(spot, GRID), :] * BRANCH_SCALE
                mixed = mixed.astype(jnp.bfloat16)
                mbconv_ref[pl.ds(spot, GRID), :] = mixed
                mixed = mixed.astype(jnp.float32)
                center = jnp.mean(mixed, axis=-1, keepdims=True)
                moved = mixed - center
                spread = jnp.mean(moved * moved, axis=-1, keepdims=True)
                to = item * members + rb * GRID
                normed_ref[to : to + GRID, :] = (
                    moved * lax.rsqrt(spread + 1e-05) * gain
                ).astype(jnp.bfloat16)


def mbconv_half(far, span, stride_rows, owners, place, up, down, ordered, own, weights):
    rows, _, channels = ordered.shape
    hidden = weights[0].shape[1]
    count = rows * span * GRID
    part = (span + 2) * GRID
    mbconv, *normed = call(
        functools.partial(mbconv_kernel, far=far, span=span, stride_rows=stride_rows),
        place,
        [up, down, ordered, own, *weights],
        [(count, channels)] + [(count // owners, channels)] * owners,
        4 * count * channels * hidden,
        8 * MIB,
        [
            pltpu.VMEM((2, 2, part, BLOCK), jnp.float32),
            pltpu.VMEM((count, BLOCK), jnp.bfloat16),
            pltpu.VMEM((count, BLOCK), jnp.bfloat16),
            pltpu.VMEM((count, channels), jnp.float32),
        ],
    )
    return mbconv, normed


def attend_kernel(place_ref, *refs, per, far, count):
    x_refs = refs[:count]
    attend_ref, output_ref = refs[-2 - count - far], refs[-1 - count - far]
    out_refs = refs[-count - far :][:count]
    channels = x_refs[0].shape[1]
    scale = LOG2E / math.sqrt(HEAD_DIM)
    fold = LANES // HEAD_DIM
    kv_ref = refs[-1] if far else refs[count]
    members = kv_ref.shape[1]
    key_lane = lax.broadcasted_iota(jnp.int32, (members, LANES), 1) // HEAD_DIM
    query_lane = lax.broadcasted_iota(jnp.int32, (count * per, LANES), 1) // HEAD_DIM
    ones = jnp.ones((members, LANES), jnp.bfloat16)

    def step(item, carry):
        spot = pl.ds(pl.multiple_of(item * per, per), per)
        x = jnp.concatenate([ref[spot, :] for ref in x_refs], axis=0)
        if far:
            everything = jnp.concatenate(
                [x] + [ref[spot, :] for ref in refs[count : -2 - count - far]], axis=0
            )
            for begin in range(0, 2 * channels, BLOCK):
                kv_ref[item, :, begin : begin + BLOCK] = jnp.dot(
                    everything,
                    attend_ref[:, channels + begin : channels + begin + BLOCK],
                    preferred_element_type=jnp.float32,
                ).astype(jnp.bfloat16)
        queries = [
            jnp.dot(x, attend_ref[:, begin : begin + BLOCK], preferred_element_type=jnp.float32)
            for begin in range(0, channels, BLOCK)
        ]
        tiles = []
        for begin in range(0, channels, LANES):
            query = queries[begin // BLOCK][:, begin % BLOCK : begin % BLOCK + LANES]
            query = (query * scale).astype(jnp.bfloat16)
            key = kv_ref[item, :, begin : begin + LANES]
            value = kv_ref[item, :, channels + begin : channels + begin + LANES]
            upper = None
            for head in range(fold):
                key_head = jnp.where(key_lane == head, key, jnp.zeros_like(key))
                value_head = jnp.where(key_lane == head, value, jnp.zeros_like(value))
                scores = lax.dot_general(
                    query, key_head, (((1,), (1,)), ((), ())), preferred_element_type=jnp.float32
                )
                top = jnp.max(scores, axis=-1, keepdims=True)
                weight = jnp.exp2(scores - top).astype(jnp.bfloat16)
                mixed = jnp.dot(
                    weight,
                    jnp.concatenate([value_head, ones], axis=1),
                    preferred_element_type=jnp.float32,
                )
                if upper is None:
                    upper, lower = mixed[:, :LANES], mixed[:, LANES:]
                else:
                    upper = upper + mixed[:, :LANES]
                    lower = jnp.where(query_lane == head, mixed[:, LANES:], lower)
            tiles.append((upper / lower).astype(jnp.bfloat16))
        heads_out = jnp.concatenate(tiles, axis=1)
        result = jnp.dot(heads_out, output_ref[...], preferred_element_type=jnp.float32)
        result = result.astype(jnp.bfloat16)
        for index, ref in enumerate(out_refs):
            ref[spot, :] = result[index * per : (index + 1) * per]
        return carry

    lax.fori_loop(0, x_refs[0].shape[0] // per, step, 0)


def attend_half(place, pieces, others, far, per, attend_weight, output_weight):
    size, channels = pieces[0].shape
    items = size // per
    members = 2 * len(pieces) * per
    shapes = [p.shape for p in pieces]
    if far:
        shapes.append((items, members, 2 * channels))
    return call(
        functools.partial(attend_kernel, per=per, far=far, count=len(pieces)),
        place,
        [*pieces, *others, attend_weight, output_weight],
        shapes,
        items * members * channels * (4 * channels + 4 * members),
        8 * MIB,
    )


def add_kernel(place_ref, mbconv_ref, *refs):
    *back_refs, keep_ref, send_ref = refs
    owners = len(back_refs)
    channels = mbconv_ref.shape[1]
    is_left = place_ref[0] == 0
    for k, back_ref in enumerate(back_refs):
        size = back_ref.shape[0]
        base = ((place_ref[1] % owners) ^ k) * size
        for at in range(0, size, 2 * GRID):
            spot = pl.multiple_of(base + at, 2 * GRID)
            total = (
                back_ref[at : at + 2 * GRID, :].astype(jnp.float32)
                + mbconv_ref[pl.ds(spot, 2 * GRID), :].astype(jnp.float32)
            ).reshape(2, 2, SUBLANES, channels)
            left = total[:, 0].reshape(GRID, channels)
            right = total[:, 1].reshape(GRID, channels)
            to = pl.ds(pl.multiple_of(spot // 2, GRID), GRID)
            keep_ref[to, :] = jnp.where(is_left, left, right).astype(jnp.bfloat16)
            send_ref[to, :] = jnp.where(is_left, right, left).astype(jnp.bfloat16)


def add_half(place, mbconv, backs):
    count, channels = mbconv.shape
    return call(
        add_kernel, place, [mbconv, *backs], [(count // 2, channels)] * 2,
        count * channels * 64, 4 * MIB,
    )


def finish_kernel(place_ref, keep_ref, got_ref, *rest, far, owners, span, stride_rows):
    spot_half = place_ref[1] // owners
    half_at = 1 - spot_half if far else spot_half
    out_ref, placed_ref, sems = rest[-3:]
    count, channels = keep_ref.shape
    length = count // stride_rows
    row_blocks = length // (span * SUBLANES)
    at = lax.broadcasted_iota(jnp.int32, (length, length), 0)
    b = at % span
    a = (at // span) % SUBLANES
    rb = at // (span * SUBLANES)
    source = (b * row_blocks + rb) * SUBLANES + a
    select = lax.broadcasted_iota(jnp.int32, (length, length), 1) == source
    select = select.astype(jnp.bfloat16)
    copies = []
    for hm in range(stride_rows):
        for ref, which in ((keep_ref, place_ref[0]), (got_ref, 1 - place_ref[0])):
            placed = jnp.dot(
                select, ref[hm * length : (hm + 1) * length, :], preferred_element_type=jnp.float32
            ).astype(jnp.bfloat16)
            placed = placed.reshape(row_blocks, SUBLANES, span, channels)
            for rb_at in range(row_blocks):
                placed_ref[rb_at * stride_rows + hm, :, which] = placed[rb_at]
        for rb_at in range(row_blocks):
            row = rb_at * stride_rows + hm
            copies.append(
                pltpu.make_async_copy(
                    placed_ref.at[row], out_ref.at[row, :, :, half_at], sems.at[row]
                )
            )
            copies[-1].start()
    for copy in copies:
        copy.wait()


def finish_half(place, keep, got, previous, far, owners, rows, stride_rows, span):
    channels = keep.shape[1]
    anywhere = pl.BlockSpec(memory_space=pl.ANY)
    operands = [keep, got]
    previous = [] if previous is None else [previous]
    return pl.pallas_call(
        functools.partial(
            finish_kernel, far=far, owners=owners, span=span, stride_rows=stride_rows
        ),
        in_specs=[SMEM, VMEM, VMEM] + [anywhere] * len(previous),
        out_specs=anywhere,
        out_shape=jax.ShapeDtypeStruct((rows, SUBLANES, 2, HALVES, span, channels), jnp.bfloat16),
        scratch_shapes=[
            pltpu.VMEM((rows, SUBLANES, 2, span, channels), jnp.bfloat16),
            pltpu.SemaphoreType.DMA((rows,)),
        ],
        input_output_aliases={3: 0} if previous else {},
        compiler_params=pltpu.CompilerParams(vmem_limit_bytes=4 * MIB),
        cost_estimate=pl.CostEstimate(
            flops=2 * keep.shape[0] * channels * 256, bytes_accessed=2 << 20, transcendentals=0
        ),
    )(place, *operands, *previous)


def fits(tokens_shape, hidden, row_count, col_count):
    rows, cols, channels = tokens_shape
    stride_rows = rows * row_count // GRID
    stride_cols = cols * col_count // GRID
    owners = row_count // HALVES
    return (
        col_count == 2
        and row_count & (row_count - 1) == 0
        and stride_rows > 0
        and rows == 2 * stride_rows
        and cols == SUBLANES * stride_cols
        and stride_cols % (2 * col_count * HALVES) == 0
        and owners % stride_rows == 0
        and stride_cols // (col_count * HALVES) % (owners // stride_rows) == 0
        and channels % BLOCK == 0
        and hidden % (2 * BLOCK) == 0
    )


def chunked(
    tokens, expand_weight, depth_kernel, project_weight, norm_gain, attend_weight, output_weight
):
    rows, cols, channels = tokens.shape
    row_count = lax.axis_size("row")
    col_count = lax.axis_size("col")
    stride_rows = rows * row_count // GRID
    stride_cols = cols * col_count // GRID
    share = stride_cols // col_count
    span = share // HALVES
    owners = row_count // HALVES
    per = rows // stride_rows * GRID
    swap = [(0, 1), (1, 0)]
    place = jnp.stack([lax.axis_index("col"), lax.axis_index("row")]).astype(jnp.int32)

    up = lax.ppermute(tokens[rows - 1 :], "row", [(r, r + 1) for r in range(row_count - 1)])
    down = lax.ppermute(tokens[:1], "row", [(r + 1, r) for r in range(row_count - 1)])
    other = lax.ppermute(tokens, "col", swap)
    (ordered,) = arrange(place, [tokens], [other], stride_cols, share)
    own = expand_rows(place, ordered, expand_weight)
    halos = [lax.ppermute(row, "col", swap) for row in (up, down)]
    up, down = arrange(place, [up, down], halos, stride_cols, share)
    weights = (expand_weight, depth_kernel, project_weight, norm_gain.reshape(1, -1))

    def exchange(arrays, far):
        return [
            array
            if k + far * owners == 0
            else lax.ppermute(
                array, "row", [(r, r ^ (k + far * owners)) for r in range(row_count)]
            )
            for k, array in enumerate(arrays)
        ]

    keeps, pieces = {}, {}
    for far in (1, 0):
        keeps[far], normed = mbconv_half(
            far, span, stride_rows, owners, place, up, down, ordered, own, weights
        )
        pieces[far] = exchange(normed, far)
    backs, others = {}, pieces[0]
    for far in (1, 0):
        result = attend_half(place, pieces[far], others, far, per, attend_weight, output_weight)
        others = result[owners:]
        backs[far] = exchange(result[:owners], far)
    out = None
    for far in (0, 1):
        keep, send = add_half(place, keeps[far], backs[far])
        got = lax.ppermute(send, "col", swap)
        out = finish_half(place, keep, got, out, far, owners, rows, stride_rows, span)
    return out.reshape(rows, cols, channels)


def local(
    tokens, expand_weight, depth_kernel, project_weight, norm_gain, attend_weight, output_weight
):
    if fits(tokens.shape, expand_weight.shape[1], lax.axis_size("row"), lax.axis_size("col")):
        return chunked(
            tokens,
            expand_weight,
            depth_kernel,
            project_weight,
            norm_gain,
            attend_weight,
            output_weight,
        )
    tile_rows, tile_cols, channels = tokens.shape
    padded_in = extended(tokens, (("row", 0), ("col", 1)), 1)
    expanded = expand_tile(padded_in, expand_weight)
    total = jnp.zeros((tile_rows, tile_cols, expanded.shape[2]), jnp.float32)
    for shift_row in range(3):
        for shift_col in range(3):
            total = (
                total
                + expanded[
                    shift_row : shift_row + tile_rows, shift_col : shift_col + tile_cols
                ].astype(jnp.float32)
                * depth_kernel[shift_row, shift_col]
            )
    depth = gelu_tanh(total).astype(jnp.bfloat16)
    branch = jnp.dot(
        depth.reshape(tile_rows * tile_cols, -1), project_weight, preferred_element_type=jnp.float32
    )
    mbconv = (tokens.astype(jnp.float32) + branch.reshape(tile_rows, tile_cols, channels)).astype(
        jnp.bfloat16
    )
    normed = layer_norm(mbconv, norm_gain)
    row_count = lax.axis_size("row")
    col_count = lax.axis_size("col")
    devices = row_count * col_count
    stride_rows = tile_rows * row_count // GRID
    stride_cols = tile_cols * col_count // GRID
    col_blocks = tile_cols // stride_cols
    if row_count % GRID == 0:
        spread_count = stride_rows // tile_rows
        per_dest = tile_rows * stride_cols // devices
        ordered = normed.reshape(tile_rows, col_blocks, stride_cols, channels).transpose(0, 2, 1, 3)
        ordered = ordered.reshape(devices, per_dest, col_blocks, channels)
    else:
        spread_count = 1
        row_blocks = tile_rows // stride_rows
        ordered = normed.reshape(
            row_blocks, stride_rows, col_blocks, stride_cols, channels
        ).transpose(1, 3, 0, 2, 4)
        ordered = ordered.reshape(devices, -1, row_blocks * col_blocks, channels)
    piece = lax.all_to_all(ordered, ("row", "col"), split_axis=0, concat_axis=0, tiled=True)
    items = piece.shape[1]
    per_source = piece.shape[2]
    grouped = piece.reshape(
        row_count // spread_count, spread_count, col_count, items, per_source, channels
    )
    grouped = grouped.transpose(3, 1, 0, 2, 4, 5).reshape(items * spread_count, -1, channels)
    result = attend_groups(grouped, attend_weight, output_weight)
    result = result.reshape(
        items, spread_count, row_count // spread_count, col_count, per_source, channels
    )
    returned = lax.all_to_all(
        result.transpose(2, 1, 3, 0, 4, 5).reshape(devices, items, per_source, channels),
        ("row", "col"),
        split_axis=0,
        concat_axis=0,
        tiled=True,
    )
    if row_count % GRID == 0:
        attention = returned.reshape(tile_rows, stride_cols, col_blocks, channels).transpose(
            0, 2, 1, 3
        )
    else:
        row_blocks = tile_rows // stride_rows
        attention = returned.reshape(
            stride_rows, stride_cols, row_blocks, col_blocks, channels
        ).transpose(2, 0, 3, 1, 4)
    attention = attention.reshape(tile_rows, tile_cols, channels)
    return (mbconv.astype(jnp.float32) + attention.astype(jnp.float32)).astype(jnp.bfloat16)


def solution(mesh):
    placed = (P(("parts", "row"), "col", None), P(), P(), P(), P(), P(), P())

    return jax.shard_map(
        local,
        mesh=mesh,
        in_specs=placed,
        out_specs=P(("parts", "row"), "col", None),
        check_vma=False,
    )
```

```python
import functools
import math

import jax
import jax.numpy as jnp
from jax import lax
from jax.experimental import pallas as pl
from jax.experimental.pallas import tpu as pltpu
from jax.sharding import PartitionSpec as P


HEADS = 16
HEAD_DIM = 32
GRID = 16
HALVES = 2
SUBLANES = 8
LANES = 128
LOG2E = 1.4426950408889634
BLOCK = 256
GELU_ONE = math.sqrt(2 / math.pi)
GELU_THREE = 0.044715 * GELU_ONE
CUBE_ROOT = GELU_THREE ** (1 / 3)
TAP_SCALE = 0.5 * CUBE_ROOT
BRANCH_SCALE = 0.5 / CUBE_ROOT


def extended(cells, sides, width):
    for axis, dim in sides:
        count = lax.axis_size(axis)
        ends = count - 1
        head = lax.slice_in_dim(cells, 0, width, axis=dim)
        tail = lax.slice_in_dim(cells, cells.shape[dim] - width, cells.shape[dim], axis=dim)
        cells = jnp.concatenate(
            [
                lax.ppermute(tail, axis, [(i, (i + 1) % count) for i in range(ends)]),
                cells,
                lax.ppermute(head, axis, [((i + 1) % count, i) for i in range(ends)]),
            ],
            axis=dim,
        )
    return cells


def gelu_tanh(values):
    return jax.nn.gelu(values, approximate=True)


def gelu_twice(v):
    return v + v * jnp.tanh(v * (GELU_ONE + GELU_THREE * (v * v)))


def gelu_scaled(w):
    return w + w * jnp.tanh(w * (GELU_ONE / CUBE_ROOT + w * w))


def expand_tile(inputs, expand_weight):
    shape = inputs.shape
    product = jnp.dot(
        inputs.reshape(-1, shape[2]), expand_weight, preferred_element_type=jnp.float32
    )
    return gelu_tanh(product).astype(jnp.bfloat16).reshape(shape[0], shape[1], -1)


def layer_norm(values, gain):
    values = values.astype(jnp.float32)
    center = jnp.mean(values, axis=-1, keepdims=True)
    spread = jnp.mean((values - center) ** 2, axis=-1, keepdims=True)
    return ((values - center) * lax.rsqrt(spread + 1e-05) * gain).astype(jnp.bfloat16)


def attend_groups(groups, attend_weight, output_weight):
    count, members, channels = groups.shape
    projected = jnp.dot(
        groups.reshape(count * members, channels), attend_weight, preferred_element_type=jnp.float32
    )
    projected = projected.astype(jnp.bfloat16).reshape(count, members, 3, HEADS, HEAD_DIM)
    query_heads = projected[:, :, 0]
    key_heads = projected[:, :, 1]
    value_heads = projected[:, :, 2]
    scores = jnp.einsum(
        "nqhd,nkhd->nhqk", query_heads, key_heads, preferred_element_type=jnp.float32
    ) / math.sqrt(HEAD_DIM)
    soft = jax.nn.softmax(scores, axis=-1).astype(jnp.bfloat16)
    heads_out = jnp.einsum("nhqk,nkhd->nqhd", soft, value_heads, preferred_element_type=jnp.float32)
    heads_out = heads_out.astype(jnp.bfloat16).reshape(count * members, channels)
    result = jnp.dot(heads_out, output_weight, preferred_element_type=jnp.float32).astype(
        jnp.bfloat16
    )
    return result.reshape(count, members, channels)


def arrange_kernel(
    place_ref, own_ref, other_ref, ordered_ref, far_ref, near_ref, *, stride_cols, share, owners
):
    rows, cols, _ = own_ref.shape
    size = ordered_ref.shape[1]
    col = place_ref[0]
    at = lax.broadcasted_iota(jnp.int32, (size, cols), 0)
    want = (at % GRID) * stride_cols + at // GRID + (col * share - 1)
    index = lax.broadcasted_iota(jnp.int32, (size, cols), 1)
    select_own = (index + col * cols == want).astype(jnp.bfloat16)
    select_other = (index + (1 - col) * cols == want).astype(jnp.bfloat16)
    for row in range(rows):
        picked = jnp.dot(select_own, own_ref[row], preferred_element_type=jnp.float32) + jnp.dot(
            select_other, other_ref[row], preferred_element_type=jnp.float32
        )
        ordered_ref[row] = picked.astype(jnp.bfloat16)
    is_low = place_ref[1] < owners
    first, last = ordered_ref[0], ordered_ref[rows - 1]
    far_ref[...] = jnp.where(is_low, first, last)
    near_ref[...] = jnp.where(is_low, last, first)


VMEM = pl.BlockSpec(memory_space=pltpu.VMEM)
SMEM = pl.BlockSpec(memory_space=pltpu.SMEM)
MIB = 1 << 20


def call(kernel, place, operands, shapes, flops, limit, scratch=(), **options):
    return pl.pallas_call(
        kernel,
        in_specs=[SMEM] + [VMEM] * len(operands),
        out_specs=[VMEM] * len(shapes),
        out_shape=[jax.ShapeDtypeStruct(shape, jnp.bfloat16) for shape in shapes],
        scratch_shapes=list(scratch),
        compiler_params=pltpu.CompilerParams(vmem_limit_bytes=limit),
        cost_estimate=pl.CostEstimate(flops=flops, bytes_accessed=1 << 20, transcendentals=0),
    )(place, *operands)


def arrange(place, own, other, stride_cols, share, owners):
    rows, cols, channels = own.shape
    size = (share + 2) * GRID
    return call(
        functools.partial(arrange_kernel, stride_cols=stride_cols, share=share, owners=owners),
        place,
        [own, other],
        [(rows, size, channels), (size, channels), (size, channels)],
        4 * rows * size * cols * channels,
        8 * MIB,
    )


def expand_kernel(place_ref, ordered_ref, expand_ref, expanded_ref):
    rows = ordered_ref.shape[0]
    hidden = expand_ref.shape[1]

    def step(index, carry):
        for half in range(2):
            lanes = pl.ds(pl.multiple_of(index * 2 * BLOCK + half * BLOCK, BLOCK), BLOCK)
            for row in range(rows):
                product = jnp.dot(
                    ordered_ref[row], expand_ref[:, lanes], preferred_element_type=jnp.float32
                )
                expanded_ref[2 * index + half, row] = gelu_twice(product).astype(jnp.bfloat16)
        return carry

    lax.fori_loop(0, hidden // (2 * BLOCK), step, 0)


def expand_rows(place, ordered, expand_weight):
    rows, size, channels = ordered.shape
    hidden = expand_weight.shape[1]
    return call(
        expand_kernel,
        place,
        [ordered, expand_weight],
        [(hidden // BLOCK, rows, size, BLOCK)],
        2 * rows * size * channels * hidden,
        8 * MIB,
    )[0]


def mbconv_kernel(place_ref, *refs, far, share, stride_rows, halos, owners):
    halo_refs = refs[:halos]
    ordered_ref, own_ref, expand_ref, taps_ref, project_ref, gain_ref, mbconv_ref = refs[halos : halos + 7]
    normed_refs = refs[halos + 7 : halos + 7 + owners]
    edge_rows, depth_a, depth_b, acc = refs[halos + 7 + owners :]
    hidden = expand_ref.shape[1]
    rows = ordered_ref.shape[0]
    row_blocks = rows // stride_rows
    spot_half = place_ref[1] // owners
    half_at = 1 - spot_half if far else spot_half
    depth_b[...] = jnp.zeros_like(depth_b)
    acc[...] = jnp.zeros_like(acc)
    halo = halo_refs[0][...]
    for ref in halo_refs[1:]:
        halo = halo + ref[...]

    def step(hm, index, carry):
        for half, depth in ((0, depth_a), (1, depth_b)):
            block = 2 * index + half
            product = jnp.dot(
                halo,
                expand_ref[:, pl.ds(block * BLOCK, BLOCK)],
                preferred_element_type=jnp.float32,
            )
            edge_rows[half] = gelu_twice(product)
            if half == 0:
                acc[...] = acc[...] + jnp.dot(
                    depth_b[...],
                    project_ref[pl.ds(jnp.maximum(block - 1, 0) * BLOCK, BLOCK), :],
                    preferred_element_type=jnp.float32,
                )
            for lane in range(0, BLOCK, LANES):
                lanes = slice(lane, lane + LANES)
                taps = [
                    [
                        taps_ref[dr, dc : dc + 1, pl.ds(block * BLOCK + lane, LANES)] * TAP_SCALE
                        for dc in range(3)
                    ]
                    for dr in range(3)
                ]
                for pair in range(0, share, 2):
                    parts = {}
                    for low in range(0, GRID, SUBLANES):
                        source = []
                        for row in range(hm, rows + hm + 1):
                            tiles = []
                            for k in range(4):
                                at = (pair + k) * GRID
                                if row == 0 or row == rows + 1:
                                    at += low
                                    tiles.append(edge_rows[half, at : at + SUBLANES, lanes])
                                else:
                                    tile = own_ref[block, row - 1, at : at + GRID, lanes]
                                    tiles.append(tile.astype(jnp.float32)[low : low + SUBLANES])
                            source.append(tiles)
                        for b in (0, 1):
                            for rb in range(row_blocks):
                                total = None
                                for dr in range(3):
                                    for dc in range(3):
                                        term = source[rb * stride_rows + dr][b + dc] * taps[dr][dc]
                                        total = term if total is None else total + term
                                parts.setdefault((rb, b), []).append(gelu_scaled(total))
                    for (rb, b), tiles in parts.items():
                        spot = ((pair + b) * row_blocks + rb) * GRID
                        depth[spot : spot + GRID, lanes] = jnp.concatenate(tiles, axis=0).astype(
                            jnp.bfloat16
                        )
            if half == 0:
                acc[...] = acc[...] + jnp.dot(
                    depth_a[...],
                    project_ref[pl.ds(block * BLOCK, BLOCK), :],
                    preferred_element_type=jnp.float32,
                )
        return carry

    for hm in range(stride_rows):

        @pl.when(half_at == hm)
        def _():
            lax.fori_loop(0, hidden // (2 * BLOCK), functools.partial(step, hm), 0)

    gain = gain_ref[...]
    acc[...] = acc[...] + jnp.dot(
        depth_b[...],
        project_ref[hidden - BLOCK : hidden, :],
        preferred_element_type=jnp.float32,
    )
    members = row_blocks * GRID
    items = share // owners
    for k, normed_ref in enumerate(normed_refs):
        owner = (place_ref[1] % owners) ^ k
        for item in range(items):
            for rb in range(row_blocks):
                spot = pl.multiple_of((owner * items + item) * members + rb * GRID, GRID)
                column = pl.multiple_of((owner * items + item + 1) * GRID, GRID)
                tokens = ordered_ref[rb * stride_rows + half_at, pl.ds(column, GRID), :]
                mixed = tokens.astype(jnp.float32) + acc[pl.ds(spot, GRID), :] * BRANCH_SCALE
                mixed = mixed.astype(jnp.bfloat16)
                mbconv_ref[pl.ds(spot, GRID), :] = mixed
                mixed = mixed.astype(jnp.float32)
                center = jnp.mean(mixed, axis=-1, keepdims=True)
                moved = mixed - center
                spread = jnp.mean(moved * moved, axis=-1, keepdims=True)
                to = item * members + rb * GRID
                normed_ref[to : to + GRID, :] = (
                    moved * lax.rsqrt(spread + 1e-05) * gain
                ).astype(jnp.bfloat16)


def mbconv_half(far, share, stride_rows, owners, place, halos, ordered, own, weights):
    rows, size, channels = ordered.shape
    hidden = weights[0].shape[1]
    count = rows // stride_rows * share * GRID
    mbconv, *normed = call(
        functools.partial(
            mbconv_kernel, far=far, share=share, stride_rows=stride_rows, halos=len(halos),
            owners=owners,
        ),
        place,
        [*halos, ordered, own, *weights],
        [(count, channels)] + [(count // owners, channels)] * owners,
        4 * count * channels * hidden,
        8 * MIB,
        [
            pltpu.VMEM((2, size, BLOCK), jnp.float32),
            pltpu.VMEM((count, BLOCK), jnp.bfloat16),
            pltpu.VMEM((count, BLOCK), jnp.bfloat16),
            pltpu.VMEM((count, channels), jnp.float32),
        ],
    )
    return mbconv, normed


def attend_kernel(place_ref, *refs, per, far, count):
    x_refs = refs[:count]
    attend_ref, output_ref = refs[-2 - count - far], refs[-1 - count - far]
    out_refs = refs[-count - far :][:count]
    channels = x_refs[0].shape[1]
    scale = LOG2E / math.sqrt(HEAD_DIM)
    fold = LANES // HEAD_DIM
    kv_ref = refs[-1] if far else refs[count]
    members = kv_ref.shape[1]
    key_lane = lax.broadcasted_iota(jnp.int32, (members, LANES), 1) // HEAD_DIM
    query_lane = lax.broadcasted_iota(jnp.int32, (count * per, LANES), 1) // HEAD_DIM
    ones = jnp.ones((members, LANES), jnp.bfloat16)

    def step(item, carry):
        spot = pl.ds(pl.multiple_of(item * per, per), per)
        x = jnp.concatenate([ref[spot, :] for ref in x_refs], axis=0)
        if far:
            everything = jnp.concatenate(
                [x] + [ref[spot, :] for ref in refs[count : -2 - count - far]], axis=0
            )
            for begin in range(0, 2 * channels, BLOCK):
                kv_ref[item, :, begin : begin + BLOCK] = jnp.dot(
                    everything,
                    attend_ref[:, channels + begin : channels + begin + BLOCK],
                    preferred_element_type=jnp.float32,
                ).astype(jnp.bfloat16)
        queries = [
            jnp.dot(x, attend_ref[:, begin : begin + BLOCK], preferred_element_type=jnp.float32)
            for begin in range(0, channels, BLOCK)
        ]
        tiles = []
        for begin in range(0, channels, LANES):
            query = queries[begin // BLOCK][:, begin % BLOCK : begin % BLOCK + LANES]
            query = (query * scale).astype(jnp.bfloat16)
            key = kv_ref[item, :, begin : begin + LANES]
            value = kv_ref[item, :, channels + begin : channels + begin + LANES]
            upper = None
            for head in range(fold):
                key_head = jnp.where(key_lane == head, key, jnp.zeros_like(key))
                value_head = jnp.where(key_lane == head, value, jnp.zeros_like(value))
                scores = lax.dot_general(
                    query, key_head, (((1,), (1,)), ((), ())), preferred_element_type=jnp.float32
                )
                top = jnp.max(scores, axis=-1, keepdims=True)
                weight = jnp.exp2(scores - top).astype(jnp.bfloat16)
                mixed = jnp.dot(
                    weight,
                    jnp.concatenate([value_head, ones], axis=1),
                    preferred_element_type=jnp.float32,
                )
                if upper is None:
                    upper, lower = mixed[:, :LANES], mixed[:, LANES:]
                else:
                    upper = upper + mixed[:, :LANES]
                    lower = jnp.where(query_lane == head, mixed[:, LANES:], lower)
            tiles.append((upper / lower).astype(jnp.bfloat16))
        heads_out = jnp.concatenate(tiles, axis=1)
        result = jnp.dot(heads_out, output_ref[...], preferred_element_type=jnp.float32)
        result = result.astype(jnp.bfloat16)
        for index, ref in enumerate(out_refs):
            ref[spot, :] = result[index * per : (index + 1) * per]
        return carry

    lax.fori_loop(0, x_refs[0].shape[0] // per, step, 0)


def attend_half(place, pieces, others, far, per, attend_weight, output_weight):
    size, channels = pieces[0].shape
    items = size // per
    members = 2 * len(pieces) * per
    shapes = [p.shape for p in pieces]
    if far:
        shapes.append((items, members, 2 * channels))
    return call(
        functools.partial(attend_kernel, per=per, far=far, count=len(pieces)),
        place,
        [*pieces, *others, attend_weight, output_weight],
        shapes,
        items * members * channels * (4 * channels + 4 * members),
        8 * MIB,
    )


def add_kernel(place_ref, *refs, owners):
    halves = len(refs) // (1 + owners)
    keep_ref, send_ref = refs[-2:]
    is_left = place_ref[0] == 0
    for half in range(halves):
        mbconv_ref = refs[half]
        channels = mbconv_ref.shape[1]
        for k in range(owners):
            back_ref = refs[halves + half * owners + k]
            size = back_ref.shape[0]
            base = ((place_ref[1] % owners) ^ k) * size
            for at in range(0, size, 2 * GRID):
                spot = pl.multiple_of(base + at, 2 * GRID)
                total = (
                    back_ref[at : at + 2 * GRID, :].astype(jnp.float32)
                    + mbconv_ref[pl.ds(spot, 2 * GRID), :].astype(jnp.float32)
                ).reshape(2, 2, SUBLANES, channels)
                left = total[:, 0].reshape(GRID, channels)
                right = total[:, 1].reshape(GRID, channels)
                to = pl.ds(pl.multiple_of(spot // 2, GRID), GRID)
                keep_ref[half, to, :] = jnp.where(is_left, left, right).astype(jnp.bfloat16)
                send_ref[half, to, :] = jnp.where(is_left, right, left).astype(jnp.bfloat16)


def add_halves(place, mbconvs, backs):
    count, channels = mbconvs[0].shape
    return call(
        functools.partial(add_kernel, owners=len(backs[0])),
        place,
        [*mbconvs, *backs[0], *backs[1]],
        [(len(mbconvs), count // 2, channels)] * 2,
        count * channels * 64,
        6 * MIB,
    )


def finish_kernel(place_ref, ready_ref, *rest, mine, owners):
    out_ref, placed_ref, sems = rest[-3:]
    halves, length, _ = ready_ref.shape
    row_blocks, _, blocks, _, share, channels = out_ref.shape
    which = place_ref[0] if mine else 1 - place_ref[0]
    at = lax.broadcasted_iota(jnp.int32, (length, length), 0)
    b = at % share
    a = (at // share) % blocks
    rb = at // (share * blocks)
    source = (b * row_blocks + rb) * blocks + a
    select = lax.broadcasted_iota(jnp.int32, (length, length), 1) == source
    select = select.astype(jnp.bfloat16)
    copies = []
    for half in range(halves):
        hm = place_ref[1] // owners if half == 0 else 1 - place_ref[1] // owners
        placed = jnp.dot(select, ready_ref[half], preferred_element_type=jnp.float32)
        placed_ref[half] = placed.astype(jnp.bfloat16).reshape(row_blocks, blocks, share, channels)
        for rb_at in range(row_blocks):
            copies.append(
                pltpu.make_async_copy(
                    placed_ref.at[half, rb_at],
                    out_ref.at[rb_at, hm, :, which],
                    sems.at[half, rb_at],
                )
            )
            copies[-1].start()
    for copy in copies:
        copy.wait()


def finish(place, ready, previous, mine, owners, shape):
    anywhere = pl.BlockSpec(memory_space=pl.ANY)
    row_blocks, stride_rows, blocks, _, share, channels = shape
    previous = [] if previous is None else [previous]
    return pl.pallas_call(
        functools.partial(finish_kernel, mine=mine, owners=owners),
        in_specs=[SMEM, VMEM] + [anywhere] * len(previous),
        out_specs=anywhere,
        out_shape=jax.ShapeDtypeStruct(shape, jnp.bfloat16),
        scratch_shapes=[
            pltpu.VMEM((stride_rows, row_blocks, blocks, share, channels), jnp.bfloat16),
            pltpu.SemaphoreType.DMA((stride_rows, row_blocks)),
        ],
        input_output_aliases={2: 0} if previous else {},
        compiler_params=pltpu.CompilerParams(vmem_limit_bytes=6 * MIB),
        cost_estimate=pl.CostEstimate(
            flops=4 * ready.size * 256, bytes_accessed=1 << 20, transcendentals=0
        ),
    )(place, ready, *previous)


def fits(tokens_shape, hidden, row_count, col_count):
    rows, cols, channels = tokens_shape
    stride_rows = rows * row_count // GRID
    stride_cols = cols * col_count // GRID
    owners = row_count // HALVES
    return (
        col_count == 2
        and row_count & (row_count - 1) == 0
        and stride_rows == HALVES
        and rows == 2 * stride_rows
        and cols == SUBLANES * stride_cols
        and stride_cols % (2 * col_count * owners) == 0
        and channels % BLOCK == 0
        and hidden % (2 * BLOCK) == 0
    )


def chunked(
    tokens, expand_weight, depth_kernel, project_weight, norm_gain, attend_weight, output_weight
):
    rows, cols, channels = tokens.shape
    row_count = lax.axis_size("row")
    col_count = lax.axis_size("col")
    stride_rows = rows * row_count // GRID
    stride_cols = cols * col_count // GRID
    share = stride_cols // col_count
    owners = row_count // HALVES
    per = rows // stride_rows * GRID
    swap = [(0, 1), (1, 0)]
    place = jnp.stack([lax.axis_index("col"), lax.axis_index("row")]).astype(jnp.int32)

    other = lax.ppermute(tokens, "col", swap)
    ordered, to_ends, to_middle = arrange(place, tokens, other, stride_cols, share, owners)
    outward = [(r, r - 1) for r in range(1, owners)]
    outward += [(r, r + 1) for r in range(owners, row_count - 1)]
    far_halos = [
        lax.ppermute(to_middle, "row", [(owners - 1, owners), (owners, owners - 1)]),
        lax.ppermute(to_ends, "row", outward),
    ]
    own = expand_rows(place, ordered, expand_weight)
    near_halos = [lax.ppermute(to_middle, "row", [(t, f) for f, t in outward])]
    weights = (expand_weight, depth_kernel, project_weight, norm_gain.reshape(1, -1))

    def exchange(arrays, far):
        return [
            array
            if k + far * owners == 0
            else lax.ppermute(
                array, "row", [(r, r ^ (k + far * owners)) for r in range(row_count)]
            )
            for k, array in enumerate(arrays)
        ]

    keeps, pieces = {}, {}
    for far in (1, 0):
        keeps[far], normed = mbconv_half(
            far, share, stride_rows, owners, place,
            far_halos if far else near_halos, ordered, own, weights,
        )
        pieces[far] = exchange(normed, far)
    backs, others = {}, pieces[0]
    for far in (1, 0):
        result = attend_half(place, pieces[far], others, far, per, attend_weight, output_weight)
        others = result[owners:]
        backs[far] = exchange(result[:owners], far)
    keep, send = add_halves(place, (keeps[0], keeps[1]), (backs[0], backs[1]))
    got = lax.ppermute(send, "col", swap)
    shape = (rows // stride_rows, stride_rows, cols // stride_cols, col_count, share, channels)
    out = finish(place, keep, None, True, owners, shape)
    out = finish(place, got, out, False, owners, shape)
    return out.reshape(rows, cols, channels)


def local(
    tokens, expand_weight, depth_kernel, project_weight, norm_gain, attend_weight, output_weight
):
    if fits(tokens.shape, expand_weight.shape[1], lax.axis_size("row"), lax.axis_size("col")):
        return chunked(
            tokens,
            expand_weight,
            depth_kernel,
            project_weight,
            norm_gain,
            attend_weight,
            output_weight,
        )
    tile_rows, tile_cols, channels = tokens.shape
    padded_in = extended(tokens, (("row", 0), ("col", 1)), 1)
    expanded = expand_tile(padded_in, expand_weight)
    total = jnp.zeros((tile_rows, tile_cols, expanded.shape[2]), jnp.float32)
    for shift_row in range(3):
        for shift_col in range(3):
            total = (
                total
                + expanded[
                    shift_row : shift_row + tile_rows, shift_col : shift_col + tile_cols
                ].astype(jnp.float32)
                * depth_kernel[shift_row, shift_col]
            )
    depth = gelu_tanh(total).astype(jnp.bfloat16)
    branch = jnp.dot(
        depth.reshape(tile_rows * tile_cols, -1), project_weight, preferred_element_type=jnp.float32
    )
    mbconv = (tokens.astype(jnp.float32) + branch.reshape(tile_rows, tile_cols, channels)).astype(
        jnp.bfloat16
    )
    normed = layer_norm(mbconv, norm_gain)
    row_count = lax.axis_size("row")
    col_count = lax.axis_size("col")
    devices = row_count * col_count
    stride_rows = tile_rows * row_count // GRID
    stride_cols = tile_cols * col_count // GRID
    col_blocks = tile_cols // stride_cols
    if row_count % GRID == 0:
        spread_count = stride_rows // tile_rows
        per_dest = tile_rows * stride_cols // devices
        ordered = normed.reshape(tile_rows, col_blocks, stride_cols, channels).transpose(0, 2, 1, 3)
        ordered = ordered.reshape(devices, per_dest, col_blocks, channels)
    else:
        spread_count = 1
        row_blocks = tile_rows // stride_rows
        ordered = normed.reshape(
            row_blocks, stride_rows, col_blocks, stride_cols, channels
        ).transpose(1, 3, 0, 2, 4)
        ordered = ordered.reshape(devices, -1, row_blocks * col_blocks, channels)
    piece = lax.all_to_all(ordered, ("row", "col"), split_axis=0, concat_axis=0, tiled=True)
    items = piece.shape[1]
    per_source = piece.shape[2]
    grouped = piece.reshape(
        row_count // spread_count, spread_count, col_count, items, per_source, channels
    )
    grouped = grouped.transpose(3, 1, 0, 2, 4, 5).reshape(items * spread_count, -1, channels)
    result = attend_groups(grouped, attend_weight, output_weight)
    result = result.reshape(
        items, spread_count, row_count // spread_count, col_count, per_source, channels
    )
    returned = lax.all_to_all(
        result.transpose(2, 1, 3, 0, 4, 5).reshape(devices, items, per_source, channels),
        ("row", "col"),
        split_axis=0,
        concat_axis=0,
        tiled=True,
    )
    if row_count % GRID == 0:
        attention = returned.reshape(tile_rows, stride_cols, col_blocks, channels).transpose(
            0, 2, 1, 3
        )
    else:
        row_blocks = tile_rows // stride_rows
        attention = returned.reshape(
            stride_rows, stride_cols, row_blocks, col_blocks, channels
        ).transpose(2, 0, 3, 1, 4)
    attention = attention.reshape(tile_rows, tile_cols, channels)
    return (mbconv.astype(jnp.float32) + attention.astype(jnp.float32)).astype(jnp.bfloat16)


def solution(mesh):
    placed = (P(("parts", "row"), "col", None), P(), P(), P(), P(), P(), P())

    return jax.shard_map(
        local,
        mesh=mesh,
        in_specs=placed,
        out_specs=P(("parts", "row"), "col", None),
        check_vma=False,
    )
```

```python
import functools
import math

import jax
import jax.numpy as jnp
from jax import lax
from jax.experimental import pallas as pl
from jax.experimental.pallas import tpu as pltpu
from jax.sharding import PartitionSpec as P


HEADS = 16
HEAD_DIM = 32
GRID = 16
HALVES = 2
SUBLANES = 8
LANES = 128
LOG2E = 1.4426950408889634
BLOCK = 256
GELU_ONE = math.sqrt(2 / math.pi)
GELU_THREE = 0.044715 * GELU_ONE
CUBE_ROOT = GELU_THREE ** (1 / 3)
TAP_SCALE = 0.5 * CUBE_ROOT
BRANCH_SCALE = 0.5 / CUBE_ROOT


def extended(cells, sides, width):
    for axis, dim in sides:
        count = lax.axis_size(axis)
        ends = count - 1
        head = lax.slice_in_dim(cells, 0, width, axis=dim)
        tail = lax.slice_in_dim(cells, cells.shape[dim] - width, cells.shape[dim], axis=dim)
        cells = jnp.concatenate(
            [
                lax.ppermute(tail, axis, [(i, (i + 1) % count) for i in range(ends)]),
                cells,
                lax.ppermute(head, axis, [((i + 1) % count, i) for i in range(ends)]),
            ],
            axis=dim,
        )
    return cells


def gelu_tanh(values):
    return jax.nn.gelu(values, approximate=True)


def gelu_twice(v):
    return v + v * jnp.tanh(v * (GELU_ONE + GELU_THREE * (v * v)))


def gelu_scaled(w):
    return w + w * jnp.tanh(w * (GELU_ONE / CUBE_ROOT + w * w))


def expand_tile(inputs, expand_weight):
    shape = inputs.shape
    product = jnp.dot(
        inputs.reshape(-1, shape[2]), expand_weight, preferred_element_type=jnp.float32
    )
    return gelu_tanh(product).astype(jnp.bfloat16).reshape(shape[0], shape[1], -1)


def layer_norm(values, gain):
    values = values.astype(jnp.float32)
    center = jnp.mean(values, axis=-1, keepdims=True)
    spread = jnp.mean((values - center) ** 2, axis=-1, keepdims=True)
    return ((values - center) * lax.rsqrt(spread + 1e-05) * gain).astype(jnp.bfloat16)


def attend_groups(groups, attend_weight, output_weight):
    count, members, channels = groups.shape
    projected = jnp.dot(
        groups.reshape(count * members, channels), attend_weight, preferred_element_type=jnp.float32
    )
    projected = projected.astype(jnp.bfloat16).reshape(count, members, 3, HEADS, HEAD_DIM)
    query_heads = projected[:, :, 0]
    key_heads = projected[:, :, 1]
    value_heads = projected[:, :, 2]
    scores = jnp.einsum(
        "nqhd,nkhd->nhqk", query_heads, key_heads, preferred_element_type=jnp.float32
    ) / math.sqrt(HEAD_DIM)
    soft = jax.nn.softmax(scores, axis=-1).astype(jnp.bfloat16)
    heads_out = jnp.einsum("nhqk,nkhd->nqhd", soft, value_heads, preferred_element_type=jnp.float32)
    heads_out = heads_out.astype(jnp.bfloat16).reshape(count * members, channels)
    result = jnp.dot(heads_out, output_weight, preferred_element_type=jnp.float32).astype(
        jnp.bfloat16
    )
    return result.reshape(count, members, channels)


def pick(place_ref, source_ref, row, size, mine, stride_cols, share):
    cols = source_ref.shape[1]
    col = place_ref[0] if mine else 1 - place_ref[0]
    at = lax.broadcasted_iota(jnp.int32, (size, cols), 0)
    want = (at % GRID) * stride_cols + at // GRID + (place_ref[0] * share - 1 - col * cols)
    select = (lax.broadcasted_iota(jnp.int32, (size, cols), 1) == want).astype(jnp.bfloat16)
    return jnp.dot(select, source_ref[row], preferred_element_type=jnp.float32)


def arrange_mine_kernel(place_ref, own_ref, ordered_ref, *, stride_cols, share):
    for row in range(own_ref.shape[0]):
        ordered_ref[row] = pick(
            place_ref, own_ref, row, ordered_ref.shape[1], True, stride_cols, share
        ).astype(jnp.bfloat16)


def arrange_kernel(
    place_ref, mine_ref, other_ref, ordered_ref, far_ref, near_ref, *, stride_cols, share, owners
):
    rows, size, _ = ordered_ref.shape
    for row in range(rows):
        picked = pick(place_ref, other_ref, row, size, False, stride_cols, share)
        ordered_ref[row] = (picked + mine_ref[row].astype(jnp.float32)).astype(jnp.bfloat16)
    is_low = place_ref[1] < owners
    first, last = ordered_ref[0], ordered_ref[rows - 1]
    far_ref[...] = jnp.where(is_low, first, last)
    near_ref[...] = jnp.where(is_low, last, first)


VMEM = pl.BlockSpec(memory_space=pltpu.VMEM)
SMEM = pl.BlockSpec(memory_space=pltpu.SMEM)
MIB = 1 << 20


def call(kernel, place, operands, shapes, flops, limit, scratch=(), **options):
    return pl.pallas_call(
        kernel,
        in_specs=[SMEM] + [VMEM] * len(operands),
        out_specs=[VMEM] * len(shapes),
        out_shape=[jax.ShapeDtypeStruct(shape, jnp.bfloat16) for shape in shapes],
        scratch_shapes=list(scratch),
        compiler_params=pltpu.CompilerParams(vmem_limit_bytes=limit),
        cost_estimate=pl.CostEstimate(flops=flops, bytes_accessed=1 << 20, transcendentals=0),
    )(place, *operands)


def arrange_mine(place, own, stride_cols, share):
    rows, cols, channels = own.shape
    size = (share + 2) * GRID
    return call(
        functools.partial(arrange_mine_kernel, stride_cols=stride_cols, share=share),
        place,
        [own],
        [(rows, size, channels)],
        2 * rows * size * cols * channels,
        8 * MIB,
    )[0]


def arrange(place, mine, other, stride_cols, share, owners):
    rows, size, channels = mine.shape
    return call(
        functools.partial(arrange_kernel, stride_cols=stride_cols, share=share, owners=owners),
        place,
        [mine, other],
        [(rows, size, channels), (size, channels), (size, channels)],
        2 * rows * size * other.shape[1] * channels,
        8 * MIB,
    )


def expand_kernel(place_ref, ordered_ref, expand_ref, expanded_ref):
    rows = ordered_ref.shape[0]
    hidden = expand_ref.shape[1]

    def step(index, carry):
        for half in range(2):
            lanes = pl.ds(pl.multiple_of(index * 2 * BLOCK + half * BLOCK, BLOCK), BLOCK)
            for row in range(rows):
                product = jnp.dot(
                    ordered_ref[row], expand_ref[:, lanes], preferred_element_type=jnp.float32
                )
                expanded_ref[2 * index + half, row] = gelu_twice(product).astype(jnp.bfloat16)
        return carry

    lax.fori_loop(0, hidden // (2 * BLOCK), step, 0)


def expand_rows(place, ordered, expand_weight):
    rows, size, channels = ordered.shape
    hidden = expand_weight.shape[1]
    return call(
        expand_kernel,
        place,
        [ordered, expand_weight],
        [(hidden // BLOCK, rows, size, BLOCK)],
        2 * rows * size * channels * hidden,
        8 * MIB,
    )[0]


def mbconv_kernel(place_ref, *refs, far, part, span, stride_rows, halos, owners):
    halo_refs = refs[:halos]
    ordered_ref, own_ref, expand_ref, taps_ref, project_ref, gain_ref, mbconv_ref = refs[halos : halos + 7]
    normed_refs = refs[halos + 7 : halos + 7 + len(part)]
    edge_rows, depth_a, depth_b, acc = refs[halos + 7 + len(part) :]
    hidden = expand_ref.shape[1]
    rows = ordered_ref.shape[0]
    row_blocks = rows // stride_rows
    spot_half = place_ref[1] // owners
    half_at = 1 - spot_half if far else spot_half
    depth_b[...] = jnp.zeros_like(depth_b)
    acc[...] = jnp.zeros_like(acc)
    nearest = (place_ref[1] % owners) ^ part[0]
    begin = pl.multiple_of(nearest // len(part) * (span * GRID), GRID)
    size = edge_rows.shape[1]
    halo = halo_refs[0][pl.ds(begin, size), :]
    for ref in halo_refs[1:]:
        halo = halo + ref[pl.ds(begin, size), :]

    def step(hm, index, carry):
        for half, depth in ((0, depth_a), (1, depth_b)):
            block = 2 * index + half
            product = jnp.dot(
                halo,
                expand_ref[:, pl.ds(block * BLOCK, BLOCK)],
                preferred_element_type=jnp.float32,
            )
            edge_rows[half] = gelu_twice(product)
            if half == 0:
                acc[...] = acc[...] + jnp.dot(
                    depth_b[...],
                    project_ref[pl.ds(jnp.maximum(block - 1, 0) * BLOCK, BLOCK), :],
                    preferred_element_type=jnp.float32,
                )
            for lane in range(0, BLOCK, LANES):
                lanes = slice(lane, lane + LANES)
                taps = [
                    [
                        taps_ref[dr, dc : dc + 1, pl.ds(block * BLOCK + lane, LANES)] * TAP_SCALE
                        for dc in range(3)
                    ]
                    for dr in range(3)
                ]
                for pair in range(0, span, 2):
                    parts = {}
                    for low in range(0, GRID, SUBLANES):
                        source = []
                        for row in range(hm, rows + hm + 1):
                            tiles = []
                            for k in range(4):
                                at = (pair + k) * GRID
                                if row == 0 or row == rows + 1:
                                    at += low
                                    tiles.append(edge_rows[half, at : at + SUBLANES, lanes])
                                else:
                                    tile = own_ref[block, row - 1, pl.ds(begin + at, GRID), lanes]
                                    tiles.append(tile.astype(jnp.float32)[low : low + SUBLANES])
                            source.append(tiles)
                        for b in (0, 1):
                            for rb in range(row_blocks):
                                total = None
                                for dr in range(3):
                                    for dc in range(3):
                                        term = source[rb * stride_rows + dr][b + dc] * taps[dr][dc]
                                        total = term if total is None else total + term
                                parts.setdefault((rb, b), []).append(gelu_scaled(total))
                    for (rb, b), tiles in parts.items():
                        spot = ((pair + b) * row_blocks + rb) * GRID
                        depth[spot : spot + GRID, lanes] = jnp.concatenate(tiles, axis=0).astype(
                            jnp.bfloat16
                        )
            if half == 0:
                acc[...] = acc[...] + jnp.dot(
                    depth_a[...],
                    project_ref[pl.ds(block * BLOCK, BLOCK), :],
                    preferred_element_type=jnp.float32,
                )
        return carry

    for hm in range(stride_rows):

        @pl.when(half_at == hm)
        def _():
            lax.fori_loop(0, hidden // (2 * BLOCK), functools.partial(step, hm), 0)

    gain = gain_ref[...]
    acc[...] = acc[...] + jnp.dot(
        depth_b[...],
        project_ref[hidden - BLOCK : hidden, :],
        preferred_element_type=jnp.float32,
    )
    members = row_blocks * GRID
    items = span // len(part)
    for k, normed_ref in zip(part, normed_refs):
        owner = ((place_ref[1] % owners) ^ k) % len(part)
        for item in range(items):
            for rb in range(row_blocks):
                spot = pl.multiple_of((owner * items + item) * members + rb * GRID, GRID)
                column = pl.multiple_of(begin + (owner * items + item + 1) * GRID, GRID)
                tokens = ordered_ref[rb * stride_rows + half_at, pl.ds(column, GRID), :]
                mixed = tokens.astype(jnp.float32) + acc[pl.ds(spot, GRID), :] * BRANCH_SCALE
                mixed = mixed.astype(jnp.bfloat16)
                mbconv_ref[pl.ds(spot, GRID), :] = mixed
                mixed = mixed.astype(jnp.float32)
                center = jnp.mean(mixed, axis=-1, keepdims=True)
                moved = mixed - center
                spread = jnp.mean(moved * moved, axis=-1, keepdims=True)
                to = item * members + rb * GRID
                normed_ref[to : to + GRID, :] = (
                    moved * lax.rsqrt(spread + 1e-05) * gain
                ).astype(jnp.bfloat16)


def mbconv_part(far, part, span, stride_rows, owners, place, halos, ordered, own, weights):
    rows, _, channels = ordered.shape
    hidden = weights[0].shape[1]
    count = rows // stride_rows * span * GRID
    mbconv, *normed = call(
        functools.partial(
            mbconv_kernel, far=far, part=part, span=span, stride_rows=stride_rows,
            halos=len(halos), owners=owners,
        ),
        place,
        [*halos, ordered, own, *weights],
        [(count, channels)] + [(count // len(part), channels)] * len(part),
        4 * count * channels * hidden,
        8 * MIB,
        [
            pltpu.VMEM((2, (span + 2) * GRID, BLOCK), jnp.float32),
            pltpu.VMEM((count, BLOCK), jnp.bfloat16),
            pltpu.VMEM((count, BLOCK), jnp.bfloat16),
            pltpu.VMEM((count, channels), jnp.float32),
        ],
    )
    return mbconv, normed


def attend_kernel(place_ref, *refs, per, first, count):
    x_refs = refs[:count]
    attend_ref, output_ref = refs[-2 - count - first], refs[-1 - count - first]
    out_refs = refs[-count - first :][:count]
    channels = x_refs[0].shape[1]
    scale = LOG2E / math.sqrt(HEAD_DIM)
    fold = LANES // HEAD_DIM
    kv_ref = refs[-1] if first else refs[count]
    members = kv_ref.shape[1]
    key_lane = lax.broadcasted_iota(jnp.int32, (members, LANES), 1) // HEAD_DIM
    query_lane = lax.broadcasted_iota(jnp.int32, (count * per, LANES), 1) // HEAD_DIM

    def step(item, carry):
        spot = pl.ds(pl.multiple_of(item * per, per), per)
        x = jnp.concatenate([ref[spot, :] for ref in x_refs], axis=0)
        if first:
            everything = jnp.concatenate(
                [x] + [ref[spot, :] for ref in refs[count : -2 - count - first]], axis=0
            )
            for begin in range(0, 2 * channels, BLOCK):
                kv_ref[item, :, begin : begin + BLOCK] = jnp.dot(
                    everything,
                    attend_ref[:, channels + begin : channels + begin + BLOCK],
                    preferred_element_type=jnp.float32,
                ).astype(jnp.bfloat16)
        queries = [
            jnp.dot(x, attend_ref[:, begin : begin + BLOCK], preferred_element_type=jnp.float32)
            for begin in range(0, channels, BLOCK)
        ]
        tiles = []
        for begin in range(0, channels, LANES):
            query = queries[begin // BLOCK][:, begin % BLOCK : begin % BLOCK + LANES]
            query = (query * scale).astype(jnp.bfloat16)
            key = kv_ref[item, :, begin : begin + LANES]
            value = kv_ref[item, :, channels + begin : channels + begin + LANES]
            stacked = jnp.concatenate(
                [jnp.where(query_lane == head, query, jnp.zeros_like(query)) for head in range(fold)],
                axis=0,
            )
            scores = lax.dot_general(
                stacked, key, (((1,), (1,)), ((), ())), preferred_element_type=jnp.float32
            )
            weight = jnp.exp2(scores - jnp.max(scores, axis=-1, keepdims=True)).astype(jnp.bfloat16)
            upper = lower = None
            for head in range(fold):
                value_head = jnp.where(
                    key_lane == head,
                    value,
                    (key_lane == (head + 1) % fold).astype(jnp.bfloat16),
                )
                mixed = jnp.dot(
                    weight[head * count * per : (head + 1) * count * per],
                    value_head,
                    preferred_element_type=jnp.float32,
                )
                if upper is None:
                    upper = lower = mixed
                else:
                    upper = jnp.where(query_lane == head, mixed, upper)
                    lower = jnp.where(query_lane == (head + 1) % fold, mixed, lower)
            lower = pltpu.roll(lower, LANES - HEAD_DIM, 1)
            tiles.append((upper / lower).astype(jnp.bfloat16))
        heads_out = jnp.concatenate(tiles, axis=1)
        result = jnp.dot(heads_out, output_ref[...], preferred_element_type=jnp.float32)
        result = result.astype(jnp.bfloat16)
        for index, ref in enumerate(out_refs):
            ref[spot, :] = result[index * per : (index + 1) * per]
        return carry

    lax.fori_loop(0, x_refs[0].shape[0] // per, step, 0)


def attend_part(place, pieces, others, first, per, attend_weight, output_weight):
    size, channels = pieces[0].shape
    items = size // per
    members = (len(pieces) + len(others)) * per if first else others[0].shape[1]
    shapes = [p.shape for p in pieces]
    if first:
        shapes.append((items, members, 2 * channels))
    return call(
        functools.partial(attend_kernel, per=per, first=first, count=len(pieces)),
        place,
        [*pieces, *others, attend_weight, output_weight],
        shapes,
        items * len(pieces) * per * channels * (8 * channels + 4 * members),
        8 * MIB,
    )


def add_kernel(place_ref, *refs, parts, owners):
    keep_ref, send_ref = refs[-2:]
    back_refs = list(refs[len(parts) : -2])
    is_left = place_ref[0] == 0
    for (far, part), mbconv_ref in zip(parts, refs):
        channels = mbconv_ref.shape[1]
        for k in part:
            back_ref = back_refs.pop(0)
            size = back_ref.shape[0]
            owner = (place_ref[1] % owners) ^ k
            for at in range(0, size, 2 * GRID):
                spot = pl.multiple_of(owner % len(part) * size + at, 2 * GRID)
                total = (
                    back_ref[at : at + 2 * GRID, :].astype(jnp.float32)
                    + mbconv_ref[pl.ds(spot, 2 * GRID), :].astype(jnp.float32)
                ).reshape(2, 2, SUBLANES, channels)
                left = total[:, 0].reshape(GRID, channels)
                right = total[:, 1].reshape(GRID, channels)
                to = pl.ds(pl.multiple_of((owner * size + at) // 2, GRID), GRID)
                keep_ref[far, to, :] = jnp.where(is_left, left, right).astype(jnp.bfloat16)
                send_ref[far, to, :] = jnp.where(is_left, right, left).astype(jnp.bfloat16)


def add_parts(place, parts, owners, mbconvs, backs):
    size, channels = backs[0][0].shape
    return call(
        functools.partial(add_kernel, parts=parts, owners=owners),
        place,
        [*mbconvs, *[b for back in backs for b in back]],
        [(HALVES, owners * size // 2, channels)] * 2,
        2 * owners * size * channels * 64,
        6 * MIB,
    )


def finish_kernel(place_ref, ready_ref, *rest, mine, owners):
    out_ref, placed_ref, sems = rest[-3:]
    halves, length, _ = ready_ref.shape
    row_blocks, _, blocks, _, share, channels = out_ref.shape
    which = place_ref[0] if mine else 1 - place_ref[0]
    at = lax.broadcasted_iota(jnp.int32, (length, length), 0)
    b = at % share
    a = (at // share) % blocks
    rb = at // (share * blocks)
    source = (b * row_blocks + rb) * blocks + a
    select = lax.broadcasted_iota(jnp.int32, (length, length), 1) == source
    select = select.astype(jnp.bfloat16)
    copies = []
    for half in range(halves):
        hm = place_ref[1] // owners if half == 0 else 1 - place_ref[1] // owners
        placed = jnp.dot(select, ready_ref[half], preferred_element_type=jnp.float32)
        placed_ref[half] = placed.astype(jnp.bfloat16).reshape(row_blocks, blocks, share, channels)
        for rb_at in range(row_blocks):
            copies.append(
                pltpu.make_async_copy(
                    placed_ref.at[half, rb_at],
                    out_ref.at[rb_at, hm, :, which],
                    sems.at[half, rb_at],
                )
            )
            copies[-1].start()
    for copy in copies:
        copy.wait()


def finish(place, ready, previous, mine, owners, shape):
    anywhere = pl.BlockSpec(memory_space=pl.ANY)
    row_blocks, stride_rows, blocks, _, share, channels = shape
    previous = [] if previous is None else [previous]
    return pl.pallas_call(
        functools.partial(finish_kernel, mine=mine, owners=owners),
        in_specs=[SMEM, VMEM] + [anywhere] * len(previous),
        out_specs=anywhere,
        out_shape=jax.ShapeDtypeStruct(shape, jnp.bfloat16),
        scratch_shapes=[
            pltpu.VMEM((stride_rows, row_blocks, blocks, share, channels), jnp.bfloat16),
            pltpu.SemaphoreType.DMA((stride_rows, row_blocks)),
        ],
        input_output_aliases={2: 0} if previous else {},
        compiler_params=pltpu.CompilerParams(vmem_limit_bytes=6 * MIB),
        cost_estimate=pl.CostEstimate(
            flops=4 * ready.size * 256, bytes_accessed=1 << 20, transcendentals=0
        ),
    )(place, ready, *previous)


def fits(tokens_shape, hidden, row_count, col_count):
    rows, cols, channels = tokens_shape
    stride_rows = rows * row_count // GRID
    stride_cols = cols * col_count // GRID
    owners = row_count // HALVES
    return (
        col_count == 2
        and row_count & (row_count - 1) == 0
        and stride_rows == HALVES
        and rows == 2 * stride_rows
        and cols == SUBLANES * stride_cols
        and owners % 2 == 0
        and stride_cols % (2 * col_count * owners) == 0
        and channels % BLOCK == 0
        and hidden % (2 * BLOCK) == 0
    )


def chunked(
    tokens, expand_weight, depth_kernel, project_weight, norm_gain, attend_weight, output_weight
):
    rows, cols, channels = tokens.shape
    row_count = lax.axis_size("row")
    col_count = lax.axis_size("col")
    stride_rows = rows * row_count // GRID
    stride_cols = cols * col_count // GRID
    share = stride_cols // col_count
    owners = row_count // HALVES
    per = rows // stride_rows * GRID
    swap = [(0, 1), (1, 0)]
    place = jnp.stack([lax.axis_index("col"), lax.axis_index("row")]).astype(jnp.int32)

    other = lax.ppermute(tokens, "col", swap)
    mine = arrange_mine(place, tokens, stride_cols, share)
    ordered, to_ends, to_middle = arrange(place, mine, other, stride_cols, share, owners)
    outward = [(r, r - 1) for r in range(1, owners)]
    outward += [(r, r + 1) for r in range(owners, row_count - 1)]
    far_halos = [
        lax.ppermute(to_middle, "row", [(owners - 1, owners), (owners, owners - 1)]),
        lax.ppermute(to_ends, "row", outward),
    ]
    own = expand_rows(place, ordered, expand_weight)
    near_halos = [lax.ppermute(to_middle, "row", [(t, f) for f, t in outward])]
    weights = (expand_weight, depth_kernel, project_weight, norm_gain.reshape(1, -1))

    def exchange(arrays, far, part):
        return [
            array
            if k + far * owners == 0
            else lax.ppermute(
                array, "row", [(r, r ^ (k + far * owners)) for r in range(row_count)]
            )
            for k, array in zip(part, arrays)
        ]

    every = tuple(range(owners))
    pair = len(every) // 2
    parts = ((1, every[:pair]), (1, every[pair:]), (0, every))
    keeps, pieces = [], []
    for far, part in parts:
        mbconv, normed = mbconv_part(
            far, part, share * len(part) // owners, stride_rows, owners, place,
            far_halos if far else near_halos, ordered, own, weights,
        )
        keeps.append(mbconv)
        pieces.append(exchange(normed, far, part))
    backs, others = [], [p for piece in pieces[1:] for p in piece]
    for index, (far, part) in enumerate(parts):
        result = attend_part(
            place, pieces[index], others, index == 0, per, attend_weight,
            output_weight,
        )
        if index == 0:
            *result, keys_values = result
            others = [keys_values]
        backs.append(exchange(result, far, part))
    keep, send = add_parts(place, parts, owners, keeps, backs)
    got = lax.ppermute(send, "col", swap)
    shape = (rows // stride_rows, stride_rows, cols // stride_cols, col_count, share, channels)
    out = finish(place, keep, None, True, owners, shape)
    out = finish(place, got, out, False, owners, shape)
    return out.reshape(rows, cols, channels)


def local(
    tokens, expand_weight, depth_kernel, project_weight, norm_gain, attend_weight, output_weight
):
    if fits(tokens.shape, expand_weight.shape[1], lax.axis_size("row"), lax.axis_size("col")):
        return chunked(
            tokens,
            expand_weight,
            depth_kernel,
            project_weight,
            norm_gain,
            attend_weight,
            output_weight,
        )
    tile_rows, tile_cols, channels = tokens.shape
    padded_in = extended(tokens, (("row", 0), ("col", 1)), 1)
    expanded = expand_tile(padded_in, expand_weight)
    total = jnp.zeros((tile_rows, tile_cols, expanded.shape[2]), jnp.float32)
    for shift_row in range(3):
        for shift_col in range(3):
            total = (
                total
                + expanded[
                    shift_row : shift_row + tile_rows, shift_col : shift_col + tile_cols
                ].astype(jnp.float32)
                * depth_kernel[shift_row, shift_col]
            )
    depth = gelu_tanh(total).astype(jnp.bfloat16)
    branch = jnp.dot(
        depth.reshape(tile_rows * tile_cols, -1), project_weight, preferred_element_type=jnp.float32
    )
    mbconv = (tokens.astype(jnp.float32) + branch.reshape(tile_rows, tile_cols, channels)).astype(
        jnp.bfloat16
    )
    normed = layer_norm(mbconv, norm_gain)
    row_count = lax.axis_size("row")
    col_count = lax.axis_size("col")
    devices = row_count * col_count
    stride_rows = tile_rows * row_count // GRID
    stride_cols = tile_cols * col_count // GRID
    col_blocks = tile_cols // stride_cols
    if row_count % GRID == 0:
        spread_count = stride_rows // tile_rows
        per_dest = tile_rows * stride_cols // devices
        ordered = normed.reshape(tile_rows, col_blocks, stride_cols, channels).transpose(0, 2, 1, 3)
        ordered = ordered.reshape(devices, per_dest, col_blocks, channels)
    else:
        spread_count = 1
        row_blocks = tile_rows // stride_rows
        ordered = normed.reshape(
            row_blocks, stride_rows, col_blocks, stride_cols, channels
        ).transpose(1, 3, 0, 2, 4)
        ordered = ordered.reshape(devices, -1, row_blocks * col_blocks, channels)
    piece = lax.all_to_all(ordered, ("row", "col"), split_axis=0, concat_axis=0, tiled=True)
    items = piece.shape[1]
    per_source = piece.shape[2]
    grouped = piece.reshape(
        row_count // spread_count, spread_count, col_count, items, per_source, channels
    )
    grouped = grouped.transpose(3, 1, 0, 2, 4, 5).reshape(items * spread_count, -1, channels)
    result = attend_groups(grouped, attend_weight, output_weight)
    result = result.reshape(
        items, spread_count, row_count // spread_count, col_count, per_source, channels
    )
    returned = lax.all_to_all(
        result.transpose(2, 1, 3, 0, 4, 5).reshape(devices, items, per_source, channels),
        ("row", "col"),
        split_axis=0,
        concat_axis=0,
        tiled=True,
    )
    if row_count % GRID == 0:
        attention = returned.reshape(tile_rows, stride_cols, col_blocks, channels).transpose(
            0, 2, 1, 3
        )
    else:
        row_blocks = tile_rows // stride_rows
        attention = returned.reshape(
            stride_rows, stride_cols, row_blocks, col_blocks, channels
        ).transpose(2, 0, 3, 1, 4)
    attention = attention.reshape(tile_rows, tile_cols, channels)
    return (mbconv.astype(jnp.float32) + attention.astype(jnp.float32)).astype(jnp.bfloat16)


def solution(mesh):
    placed = (P(("parts", "row"), "col", None), P(), P(), P(), P(), P(), P())

    return jax.shard_map(
        local,
        mesh=mesh,
        in_specs=placed,
        out_specs=P(("parts", "row"), "col", None),
        check_vma=False,
    )
```

```python
import functools
import math

import jax
import jax.numpy as jnp
from jax import lax
from jax.experimental import pallas as pl
from jax.experimental.pallas import tpu as pltpu
from jax.sharding import PartitionSpec as P


HEADS = 16
HEAD_DIM = 32
GRID = 16
HALVES = 2
SUBLANES = 8
LANES = 128
LOG2E = 1.4426950408889634
BLOCK = 256
GELU_ONE = math.sqrt(2 / math.pi)
GELU_THREE = 0.044715 * GELU_ONE
CUBE_ROOT = GELU_THREE ** (1 / 3)
TAP_SCALE = 0.5 * CUBE_ROOT
BRANCH_SCALE = 0.5 / CUBE_ROOT


def extended(cells, sides, width):
    for axis, dim in sides:
        count = lax.axis_size(axis)
        ends = count - 1
        head = lax.slice_in_dim(cells, 0, width, axis=dim)
        tail = lax.slice_in_dim(cells, cells.shape[dim] - width, cells.shape[dim], axis=dim)
        cells = jnp.concatenate(
            [
                lax.ppermute(tail, axis, [(i, (i + 1) % count) for i in range(ends)]),
                cells,
                lax.ppermute(head, axis, [((i + 1) % count, i) for i in range(ends)]),
            ],
            axis=dim,
        )
    return cells


def gelu_tanh(values):
    return jax.nn.gelu(values, approximate=True)


def gelu_twice(v):
    return v + v * jnp.tanh(v * (GELU_ONE + GELU_THREE * (v * v)))


def gelu_scaled(w):
    return w + w * jnp.tanh(w * (GELU_ONE / CUBE_ROOT + w * w))


def expand_tile(inputs, expand_weight):
    shape = inputs.shape
    product = jnp.dot(
        inputs.reshape(-1, shape[2]), expand_weight, preferred_element_type=jnp.float32
    )
    return gelu_tanh(product).astype(jnp.bfloat16).reshape(shape[0], shape[1], -1)


def layer_norm(values, gain):
    values = values.astype(jnp.float32)
    center = jnp.mean(values, axis=-1, keepdims=True)
    spread = jnp.mean((values - center) ** 2, axis=-1, keepdims=True)
    return ((values - center) * lax.rsqrt(spread + 1e-05) * gain).astype(jnp.bfloat16)


def attend_groups(groups, attend_weight, output_weight):
    count, members, channels = groups.shape
    projected = jnp.dot(
        groups.reshape(count * members, channels), attend_weight, preferred_element_type=jnp.float32
    )
    projected = projected.astype(jnp.bfloat16).reshape(count, members, 3, HEADS, HEAD_DIM)
    query_heads = projected[:, :, 0]
    key_heads = projected[:, :, 1]
    value_heads = projected[:, :, 2]
    scores = jnp.einsum(
        "nqhd,nkhd->nhqk", query_heads, key_heads, preferred_element_type=jnp.float32
    ) / math.sqrt(HEAD_DIM)
    soft = jax.nn.softmax(scores, axis=-1).astype(jnp.bfloat16)
    heads_out = jnp.einsum("nhqk,nkhd->nqhd", soft, value_heads, preferred_element_type=jnp.float32)
    heads_out = heads_out.astype(jnp.bfloat16).reshape(count * members, channels)
    result = jnp.dot(heads_out, output_weight, preferred_element_type=jnp.float32).astype(
        jnp.bfloat16
    )
    return result.reshape(count, members, channels)


def pick(place_ref, source_ref, row, size, mine, stride_cols, share):
    cols = source_ref.shape[1]
    col = place_ref[0] if mine else 1 - place_ref[0]
    at = lax.broadcasted_iota(jnp.int32, (size, cols), 0)
    want = (at % GRID) * stride_cols + at // GRID + (place_ref[0] * share - 1 - col * cols)
    select = (lax.broadcasted_iota(jnp.int32, (size, cols), 1) == want).astype(jnp.bfloat16)
    return jnp.dot(select, source_ref[row], preferred_element_type=jnp.float32)


def arrange_mine_kernel(place_ref, own_ref, ordered_ref, *, stride_cols, share):
    for row in range(own_ref.shape[0]):
        ordered_ref[row] = pick(
            place_ref, own_ref, row, ordered_ref.shape[1], True, stride_cols, share
        ).astype(jnp.bfloat16)


def arrange_kernel(
    place_ref, mine_ref, other_ref, ordered_ref, far_ref, near_ref, *, stride_cols, share, owners
):
    rows, size, _ = ordered_ref.shape
    for row in range(rows):
        picked = pick(place_ref, other_ref, row, size, False, stride_cols, share)
        ordered_ref[row] = (picked + mine_ref[row].astype(jnp.float32)).astype(jnp.bfloat16)
    is_low = place_ref[1] < owners
    first, last = ordered_ref[0], ordered_ref[rows - 1]
    far_ref[...] = jnp.where(is_low, first, last)
    near_ref[...] = jnp.where(is_low, last, first)


VMEM = pl.BlockSpec(memory_space=pltpu.VMEM)
SMEM = pl.BlockSpec(memory_space=pltpu.SMEM)
MIB = 1 << 20


def call(kernel, place, operands, shapes, flops, limit, scratch=(), kind=jnp.bfloat16):
    return pl.pallas_call(
        kernel,
        in_specs=[SMEM] + [VMEM] * len(operands),
        out_specs=[VMEM] * len(shapes),
        out_shape=[jax.ShapeDtypeStruct(shape, kind) for shape in shapes],
        scratch_shapes=list(scratch),
        compiler_params=pltpu.CompilerParams(vmem_limit_bytes=limit),
        cost_estimate=pl.CostEstimate(flops=flops, bytes_accessed=1 << 20, transcendentals=0),
    )(place, *operands)


def arrange_mine(place, own, stride_cols, share):
    rows, cols, channels = own.shape
    size = (share + 2) * GRID
    return call(
        functools.partial(arrange_mine_kernel, stride_cols=stride_cols, share=share),
        place,
        [own],
        [(rows, size, channels)],
        2 * rows * size * cols * channels,
        8 * MIB,
    )[0]


def arrange(place, mine, other, stride_cols, share, owners):
    rows, size, channels = mine.shape
    return call(
        functools.partial(arrange_kernel, stride_cols=stride_cols, share=share, owners=owners),
        place,
        [mine, other],
        [(rows, size, channels), (size, channels), (size, channels)],
        2 * rows * size * other.shape[1] * channels,
        8 * MIB,
    )


def expand_kernel(place_ref, ordered_ref, expand_ref, expanded_ref):
    rows = ordered_ref.shape[0]
    hidden = expand_ref.shape[1]

    def step(index, carry):
        for half in range(2):
            lanes = pl.ds(pl.multiple_of(index * 2 * BLOCK + half * BLOCK, BLOCK), BLOCK)
            for row in range(rows):
                product = jnp.dot(
                    ordered_ref[row], expand_ref[:, lanes], preferred_element_type=jnp.float32
                )
                expanded_ref[2 * index + half, row] = gelu_twice(product)
        return carry

    lax.fori_loop(0, hidden // (2 * BLOCK), step, 0)


def expand_rows(place, ordered, expand_weight):
    rows, size, channels = ordered.shape
    hidden = expand_weight.shape[1]
    return call(
        expand_kernel,
        place,
        [ordered, expand_weight],
        [(hidden // BLOCK, rows, size, BLOCK)],
        2 * rows * size * channels * hidden,
        8 * MIB,
        kind=jnp.float32,
    )[0]


def mbconv_kernel(place_ref, *refs, far, part, span, stride_rows, halos, owners):
    halo_refs = refs[:halos]
    ordered_ref, own_ref, expand_ref, taps_ref, project_ref, gain_ref, mbconv_ref = refs[halos : halos + 7]
    normed_refs = refs[halos + 7 : halos + 7 + len(part)]
    edge_rows, depth_a, depth_b, acc = refs[halos + 7 + len(part) :]
    hidden = expand_ref.shape[1]
    rows = ordered_ref.shape[0]
    row_blocks = rows // stride_rows
    spot_half = place_ref[1] // owners
    half_at = 1 - spot_half if far else spot_half
    depth_b[...] = jnp.zeros_like(depth_b)
    acc[...] = jnp.zeros_like(acc)
    nearest = (place_ref[1] % owners) ^ part[0]
    begin = pl.multiple_of(nearest // len(part) * (span * GRID), GRID)
    size = edge_rows.shape[1]
    halo = halo_refs[0][pl.ds(begin, size), :]
    for ref in halo_refs[1:]:
        halo = halo + ref[pl.ds(begin, size), :]

    def step(hm, index, carry):
        for half, depth in ((0, depth_a), (1, depth_b)):
            block = 2 * index + half
            product = jnp.dot(
                halo,
                expand_ref[:, pl.ds(block * BLOCK, BLOCK)],
                preferred_element_type=jnp.float32,
            )
            edge_rows[half] = gelu_twice(product)
            if half == 0:
                acc[...] = acc[...] + jnp.dot(
                    depth_b[...],
                    project_ref[pl.ds(jnp.maximum(block - 1, 0) * BLOCK, BLOCK), :],
                    preferred_element_type=jnp.float32,
                )
            for lane in range(0, BLOCK, LANES):
                lanes = slice(lane, lane + LANES)
                taps = [
                    [
                        taps_ref[dr, dc : dc + 1, pl.ds(block * BLOCK + lane, LANES)] * TAP_SCALE
                        for dc in range(3)
                    ]
                    for dr in range(3)
                ]
                for pair in range(0, span, 2):
                    parts = {}
                    for low in range(0, GRID, SUBLANES):
                        source = []
                        for row in range(hm, rows + hm + 1):
                            tiles = []
                            for k in range(4):
                                at = (pair + k) * GRID
                                if row == 0 or row == rows + 1:
                                    at += low
                                    tiles.append(edge_rows[half, at : at + SUBLANES, lanes])
                                else:
                                    at = pl.multiple_of(begin + at + low, SUBLANES)
                                    tiles.append(
                                        own_ref[block, row - 1, pl.ds(at, SUBLANES), lanes]
                                    )
                            source.append(tiles)
                        for b in (0, 1):
                            for rb in range(row_blocks):
                                total = None
                                for dr in range(3):
                                    for dc in range(3):
                                        term = source[rb * stride_rows + dr][b + dc] * taps[dr][dc]
                                        total = term if total is None else total + term
                                parts.setdefault((rb, b), []).append(gelu_scaled(total))
                    for (rb, b), tiles in parts.items():
                        spot = ((pair + b) * row_blocks + rb) * GRID
                        depth[spot : spot + GRID, lanes] = jnp.concatenate(tiles, axis=0).astype(
                            jnp.bfloat16
                        )
            if half == 0:
                acc[...] = acc[...] + jnp.dot(
                    depth_a[...],
                    project_ref[pl.ds(block * BLOCK, BLOCK), :],
                    preferred_element_type=jnp.float32,
                )
        return carry

    for hm in range(stride_rows):

        @pl.when(half_at == hm)
        def _():
            lax.fori_loop(0, hidden // (2 * BLOCK), functools.partial(step, hm), 0)

    gain = gain_ref[...]
    acc[...] = acc[...] + jnp.dot(
        depth_b[...],
        project_ref[hidden - BLOCK : hidden, :],
        preferred_element_type=jnp.float32,
    )
    members = row_blocks * GRID
    items = span // len(part)
    for k, normed_ref in zip(part, normed_refs):
        owner = ((place_ref[1] % owners) ^ k) % len(part)
        for item in range(items):
            for rb in range(row_blocks):
                spot = pl.multiple_of((owner * items + item) * members + rb * GRID, GRID)
                column = pl.multiple_of(begin + (owner * items + item + 1) * GRID, GRID)
                tokens = ordered_ref[rb * stride_rows + half_at, pl.ds(column, GRID), :]
                mixed = tokens.astype(jnp.float32) + acc[pl.ds(spot, GRID), :] * BRANCH_SCALE
                mixed = mixed.astype(jnp.bfloat16)
                mbconv_ref[pl.ds(spot, GRID), :] = mixed
                mixed = mixed.astype(jnp.float32)
                center = jnp.mean(mixed, axis=-1, keepdims=True)
                moved = mixed - center
                spread = jnp.mean(moved * moved, axis=-1, keepdims=True)
                to = item * members + rb * GRID
                normed_ref[to : to + GRID, :] = (
                    moved * lax.rsqrt(spread + 1e-05) * gain
                ).astype(jnp.bfloat16)


def mbconv_part(far, part, span, stride_rows, owners, place, halos, ordered, own, weights):
    rows, _, channels = ordered.shape
    hidden = weights[0].shape[1]
    count = rows // stride_rows * span * GRID
    mbconv, *normed = call(
        functools.partial(
            mbconv_kernel, far=far, part=part, span=span, stride_rows=stride_rows,
            halos=len(halos), owners=owners,
        ),
        place,
        [*halos, ordered, own, *weights],
        [(count, channels)] + [(count // len(part), channels)] * len(part),
        4 * count * channels * hidden,
        8 * MIB,
        [
            pltpu.VMEM((2, (span + 2) * GRID, BLOCK), jnp.float32),
            pltpu.VMEM((count, BLOCK), jnp.bfloat16),
            pltpu.VMEM((count, BLOCK), jnp.bfloat16),
            pltpu.VMEM((count, channels), jnp.float32),
        ],
    )
    return mbconv, normed


def attend_kernel(place_ref, *refs, per, first, count):
    x_refs = refs[:count]
    attend_ref, output_ref = refs[-2 - count - first], refs[-1 - count - first]
    out_refs = refs[-count - first :][:count]
    channels = x_refs[0].shape[1]
    scale = LOG2E / math.sqrt(HEAD_DIM)
    fold = LANES // HEAD_DIM
    kv_ref = refs[-1] if first else refs[count]
    members = kv_ref.shape[1]
    key_lane = lax.broadcasted_iota(jnp.int32, (members, LANES), 1) // HEAD_DIM
    query_lane = lax.broadcasted_iota(jnp.int32, (count * per, LANES), 1) // HEAD_DIM

    def attend(item):
        spot = pl.ds(pl.multiple_of(item * per, per), per)
        x = jnp.concatenate([ref[spot, :] for ref in x_refs], axis=0)
        if first:
            everything = jnp.concatenate(
                [x] + [ref[spot, :] for ref in refs[count : -2 - count - first]], axis=0
            )
            for begin in range(0, 2 * channels, BLOCK):
                kv_ref[item, :, begin : begin + BLOCK] = jnp.dot(
                    everything,
                    attend_ref[:, channels + begin : channels + begin + BLOCK],
                    preferred_element_type=jnp.float32,
                ).astype(jnp.bfloat16)
        queries = [
            jnp.dot(x, attend_ref[:, begin : begin + BLOCK], preferred_element_type=jnp.float32)
            for begin in range(0, channels, BLOCK)
        ]
        tiles = []
        for begin in range(0, channels, LANES):
            query = queries[begin // BLOCK][:, begin % BLOCK : begin % BLOCK + LANES]
            query = (query * scale).astype(jnp.bfloat16)
            key = kv_ref[item, :, begin : begin + LANES]
            value = kv_ref[item, :, channels + begin : channels + begin + LANES]
            stacked = jnp.concatenate(
                [jnp.where(query_lane == head, query, jnp.zeros_like(query)) for head in range(fold)],
                axis=0,
            )
            scores = lax.dot_general(
                stacked, key, (((1,), (1,)), ((), ())), preferred_element_type=jnp.float32
            )
            weight = jnp.exp2(scores - jnp.max(scores, axis=-1, keepdims=True)).astype(jnp.bfloat16)
            upper = lower = None
            for head in range(fold):
                value_head = jnp.where(
                    key_lane == head,
                    value,
                    (key_lane == (head + 1) % fold).astype(jnp.bfloat16),
                )
                mixed = jnp.dot(
                    weight[head * count * per : (head + 1) * count * per],
                    value_head,
                    preferred_element_type=jnp.float32,
                )
                if upper is None:
                    upper = lower = mixed
                else:
                    upper = jnp.where(query_lane == head, mixed, upper)
                    lower = jnp.where(query_lane == (head + 1) % fold, mixed, lower)
            lower = pltpu.roll(lower, LANES - HEAD_DIM, 1)
            tiles.append((upper / lower).astype(jnp.bfloat16))
        heads_out = jnp.concatenate(tiles, axis=1)
        result = jnp.dot(heads_out, output_ref[...], preferred_element_type=jnp.float32)
        result = result.astype(jnp.bfloat16)
        for index, ref in enumerate(out_refs):
            ref[spot, :] = result[index * per : (index + 1) * per]

    def step(index, carry):
        for item in range(2):
            attend(2 * index + item)
        return carry

    lax.fori_loop(0, x_refs[0].shape[0] // per // 2, step, 0)


def attend_part(place, pieces, others, first, per, attend_weight, output_weight):
    size, channels = pieces[0].shape
    items = size // per
    members = (len(pieces) + len(others)) * per if first else others[0].shape[1]
    shapes = [p.shape for p in pieces]
    if first:
        shapes.append((items, members, 2 * channels))
    return call(
        functools.partial(attend_kernel, per=per, first=first, count=len(pieces)),
        place,
        [*pieces, *others, attend_weight, output_weight],
        shapes,
        items * len(pieces) * per * channels * (8 * channels + 4 * members),
        8 * MIB,
    )


def add_kernel(place_ref, *refs, parts, owners):
    keep_ref, send_ref = refs[-2:]
    back_refs = list(refs[len(parts) : -2])
    is_left = place_ref[0] == 0
    for part, mbconv_ref in zip(parts, refs):
        channels = mbconv_ref.shape[1]
        for k in part:
            back_ref = back_refs.pop(0)
            size = back_ref.shape[0]
            owner = (place_ref[1] % owners) ^ k
            for at in range(0, size, 2 * GRID):
                spot = pl.multiple_of(owner % len(part) * size + at, 2 * GRID)
                total = (
                    back_ref[at : at + 2 * GRID, :].astype(jnp.float32)
                    + mbconv_ref[pl.ds(spot, 2 * GRID), :].astype(jnp.float32)
                ).reshape(2, 2, SUBLANES, channels)
                left = total[:, 0].reshape(GRID, channels)
                right = total[:, 1].reshape(GRID, channels)
                to = pl.ds(pl.multiple_of((owner * size + at) // 2, GRID), GRID)
                keep_ref[to, :] = jnp.where(is_left, left, right).astype(jnp.bfloat16)
                send_ref[to, :] = jnp.where(is_left, right, left).astype(jnp.bfloat16)


def add_parts(place, parts, owners, mbconvs, backs):
    size, channels = backs[0][0].shape
    return call(
        functools.partial(add_kernel, parts=parts, owners=owners),
        place,
        [*mbconvs, *[b for back in backs for b in back]],
        [(owners * size // 2, channels)] * 2,
        owners * size * channels * 64,
        6 * MIB,
    )


def finish_kernel(place_ref, ready_ref, *rest, mine, far, owners):
    out_ref, placed_ref, sems = rest[-3:]
    length, _ = ready_ref.shape
    row_blocks, _, blocks, _, share, channels = out_ref.shape
    which = place_ref[0] if mine else 1 - place_ref[0]
    hm = 1 - place_ref[1] // owners if far else place_ref[1] // owners
    at = lax.broadcasted_iota(jnp.int32, (length, length), 0)
    b = at % share
    a = (at // share) % blocks
    rb = at // (share * blocks)
    source = (b * row_blocks + rb) * blocks + a
    select = lax.broadcasted_iota(jnp.int32, (length, length), 1) == source
    placed = jnp.dot(
        select.astype(jnp.bfloat16), ready_ref[...], preferred_element_type=jnp.float32
    )
    placed = placed.astype(jnp.bfloat16).reshape(row_blocks, blocks, share, channels)
    copies = []
    for rb_at in range(row_blocks):
        placed_ref[rb_at] = placed[rb_at]
        copies.append(
            pltpu.make_async_copy(
                placed_ref.at[rb_at], out_ref.at[rb_at, hm, :, which], sems.at[rb_at]
            )
        )
        copies[-1].start()
    for copy in copies:
        copy.wait()


def finish(place, ready, previous, mine, far, owners, shape):
    anywhere = pl.BlockSpec(memory_space=pl.ANY)
    row_blocks, _, blocks, _, share, channels = shape
    previous = [] if previous is None else [previous]
    return pl.pallas_call(
        functools.partial(finish_kernel, mine=mine, far=far, owners=owners),
        in_specs=[SMEM, VMEM] + [anywhere] * len(previous),
        out_specs=anywhere,
        out_shape=jax.ShapeDtypeStruct(shape, jnp.bfloat16),
        scratch_shapes=[
            pltpu.VMEM((row_blocks, blocks, share, channels), jnp.bfloat16),
            pltpu.SemaphoreType.DMA((row_blocks,)),
        ],
        input_output_aliases={2: 0} if previous else {},
        compiler_params=pltpu.CompilerParams(vmem_limit_bytes=6 * MIB),
        cost_estimate=pl.CostEstimate(
            flops=4 * ready.size * 256, bytes_accessed=1 << 20, transcendentals=0
        ),
    )(place, ready, *previous)


def fits(tokens_shape, hidden, row_count, col_count):
    rows, cols, channels = tokens_shape
    stride_rows = rows * row_count // GRID
    stride_cols = cols * col_count // GRID
    owners = row_count // HALVES
    return (
        col_count == 2
        and row_count & (row_count - 1) == 0
        and stride_rows == HALVES
        and rows == 2 * stride_rows
        and cols == SUBLANES * stride_cols
        and owners % 2 == 0
        and stride_cols % (2 * col_count * owners) == 0
        and channels % BLOCK == 0
        and hidden % (2 * BLOCK) == 0
    )


def chunked(
    tokens, expand_weight, depth_kernel, project_weight, norm_gain, attend_weight, output_weight
):
    rows, cols, channels = tokens.shape
    row_count = lax.axis_size("row")
    col_count = lax.axis_size("col")
    stride_rows = rows * row_count // GRID
    stride_cols = cols * col_count // GRID
    share = stride_cols // col_count
    owners = row_count // HALVES
    per = rows // stride_rows * GRID
    swap = [(0, 1), (1, 0)]
    place = jnp.stack([lax.axis_index("col"), lax.axis_index("row")]).astype(jnp.int32)

    other = lax.ppermute(tokens, "col", swap)
    mine = arrange_mine(place, tokens, stride_cols, share)
    ordered, to_ends, to_middle = arrange(place, mine, other, stride_cols, share, owners)
    outward = [(r, r - 1) for r in range(1, owners)]
    outward += [(r, r + 1) for r in range(owners, row_count - 1)]
    far_halos = [
        lax.ppermute(to_middle, "row", [(owners - 1, owners), (owners, owners - 1)]),
        lax.ppermute(to_ends, "row", outward),
    ]
    own = expand_rows(place, ordered, expand_weight)
    near_halos = [lax.ppermute(to_middle, "row", [(t, f) for f, t in outward])]
    weights = (expand_weight, depth_kernel, project_weight, norm_gain.reshape(1, -1))

    def exchange(arrays, far, part):
        return [
            array
            if k + far * owners == 0
            else lax.ppermute(
                array, "row", [(r, r ^ (k + far * owners)) for r in range(row_count)]
            )
            for k, array in zip(part, arrays)
        ]

    every = tuple(range(owners))
    pair = len(every) // 2
    parts = ((1, every[:pair]), (1, every[pair:]), (0, every))
    keeps, pieces = [], []
    for far, part in parts:
        mbconv, normed = mbconv_part(
            far, part, share * len(part) // owners, stride_rows, owners, place,
            far_halos if far else near_halos, ordered, own, weights,
        )
        keeps.append(mbconv)
        pieces.append(exchange(normed, far, part))
    backs, others = [], [p for piece in pieces[1:] for p in piece]
    for index, (far, part) in enumerate(parts):
        result = attend_part(
            place, pieces[index], others, index == 0, per, attend_weight,
            output_weight,
        )
        if index == 0:
            *result, keys_values = result
            others = [keys_values]
        backs.append(exchange(result, far, part))
    shape = (rows // stride_rows, stride_rows, cols // stride_cols, col_count, share, channels)
    out = None
    for far in (1, 0):
        chosen = [i for i, (is_far, _) in enumerate(parts) if is_far == far]
        keep, send = add_parts(
            place, [parts[i][1] for i in chosen], owners,
            [keeps[i] for i in chosen], [backs[i] for i in chosen],
        )
        got = lax.ppermute(send, "col", swap)
        out = finish(place, keep, out, True, far, owners, shape)
        out = finish(place, got, out, False, far, owners, shape)
    return out.reshape(rows, cols, channels)


def local(
    tokens, expand_weight, depth_kernel, project_weight, norm_gain, attend_weight, output_weight
):
    if fits(tokens.shape, expand_weight.shape[1], lax.axis_size("row"), lax.axis_size("col")):
        return chunked(
            tokens,
            expand_weight,
            depth_kernel,
            project_weight,
            norm_gain,
            attend_weight,
            output_weight,
        )
    tile_rows, tile_cols, channels = tokens.shape
    padded_in = extended(tokens, (("row", 0), ("col", 1)), 1)
    expanded = expand_tile(padded_in, expand_weight)
    total = jnp.zeros((tile_rows, tile_cols, expanded.shape[2]), jnp.float32)
    for shift_row in range(3):
        for shift_col in range(3):
            total = (
                total
                + expanded[
                    shift_row : shift_row + tile_rows, shift_col : shift_col + tile_cols
                ].astype(jnp.float32)
                * depth_kernel[shift_row, shift_col]
            )
    depth = gelu_tanh(total).astype(jnp.bfloat16)
    branch = jnp.dot(
        depth.reshape(tile_rows * tile_cols, -1), project_weight, preferred_element_type=jnp.float32
    )
    mbconv = (tokens.astype(jnp.float32) + branch.reshape(tile_rows, tile_cols, channels)).astype(
        jnp.bfloat16
    )
    normed = layer_norm(mbconv, norm_gain)
    row_count = lax.axis_size("row")
    col_count = lax.axis_size("col")
    devices = row_count * col_count
    stride_rows = tile_rows * row_count // GRID
    stride_cols = tile_cols * col_count // GRID
    col_blocks = tile_cols // stride_cols
    if row_count % GRID == 0:
        spread_count = stride_rows // tile_rows
        per_dest = tile_rows * stride_cols // devices
        ordered = normed.reshape(tile_rows, col_blocks, stride_cols, channels).transpose(0, 2, 1, 3)
        ordered = ordered.reshape(devices, per_dest, col_blocks, channels)
    else:
        spread_count = 1
        row_blocks = tile_rows // stride_rows
        ordered = normed.reshape(
            row_blocks, stride_rows, col_blocks, stride_cols, channels
        ).transpose(1, 3, 0, 2, 4)
        ordered = ordered.reshape(devices, -1, row_blocks * col_blocks, channels)
    piece = lax.all_to_all(ordered, ("row", "col"), split_axis=0, concat_axis=0, tiled=True)
    items = piece.shape[1]
    per_source = piece.shape[2]
    grouped = piece.reshape(
        row_count // spread_count, spread_count, col_count, items, per_source, channels
    )
    grouped = grouped.transpose(3, 1, 0, 2, 4, 5).reshape(items * spread_count, -1, channels)
    result = attend_groups(grouped, attend_weight, output_weight)
    result = result.reshape(
        items, spread_count, row_count // spread_count, col_count, per_source, channels
    )
    returned = lax.all_to_all(
        result.transpose(2, 1, 3, 0, 4, 5).reshape(devices, items, per_source, channels),
        ("row", "col"),
        split_axis=0,
        concat_axis=0,
        tiled=True,
    )
    if row_count % GRID == 0:
        attention = returned.reshape(tile_rows, stride_cols, col_blocks, channels).transpose(
            0, 2, 1, 3
        )
    else:
        row_blocks = tile_rows // stride_rows
        attention = returned.reshape(
            stride_rows, stride_cols, row_blocks, col_blocks, channels
        ).transpose(2, 0, 3, 1, 4)
    attention = attention.reshape(tile_rows, tile_cols, channels)
    return (mbconv.astype(jnp.float32) + attention.astype(jnp.float32)).astype(jnp.bfloat16)


def solution(mesh):
    placed = (P(("parts", "row"), "col", None), P(), P(), P(), P(), P(), P())

    return jax.shard_map(
        local,
        mesh=mesh,
        in_specs=placed,
        out_specs=P(("parts", "row"), "col", None),
        check_vma=False,
    )
```
